32 devices in a mesh: leaf: 8 (over y, x, core), sub: 4 (over z).
Axes of the slice: x: 2, y: 2, z: 4, core: 2. Of those that a mesh axis runs over, the one named last changes fastest.
Arguments:
- currents: float32 [65536, 128], P(('leaf', 'sub')), may hold values from -6 to 6
- leaf_basis: float32 [512, 128, 128], P(('leaf', 'sub')), may hold values from -0.5 to 0.5
- leaf_rank: int32 [512], P(('leaf', 'sub')), may hold values from 64 to 128
- leaf_transfer: float32 [512, 128, 128], P(('leaf', 'sub')), may hold values from -0.25 to 0.25
- top_transfer: float32 [8, 4, 128, 128], P('leaf', None, None, 'sub'), may hold values from -0.375 to 0.375
- far_table: float32 [32, 2, 128, 128], replicated, may hold values from -0.125 to 0.125
- send_src: int32 [32, 3, 4, 12], P(('leaf', 'sub')), may hold values from -1 to 15, as said below
- recv_tgt: int32 [32, 3, 4, 12], P(('leaf', 'sub')), may hold values from -1 to 15, as said below
- recv_type: int32 [32, 3, 4, 12], P(('leaf', 'sub')), may hold values from 0 to 31, as said below
- top_coupling: float32 [8, 4, 2, 128, 128], P('leaf', None, None, 'sub'), may hold values from -0.1875 to 0.1875
- top_list: int32 [8, 4], P('leaf'), may hold values from 0 to 7, as said below
- near_blocks: float32 [2048, 2, 128, 128], P(('leaf', 'sub')), may hold values from -0.1875 to 0.1875
- near_tgt: int32 [32, 64], P(('leaf', 'sub')), may hold values from 0 to 15, as said below
- near_src: int32 [32, 64], P(('leaf', 'sub')), may hold values from 0 to 23, as said below
Outputs:
- potential: float32 [65536, 128], P(('leaf', 'sub'))
The draws below stay inside these ranges and needn't reach their ends.
Inputs may be any that keep to these rules, and one draw needn't show every extreme that they name: `send_src`: entry [q, o, s, j] names the leaf of device q (counted from its first leaf) whose coefficients fill slot j of what device q sends to device (q // 4 + o - 1) * 4 + s, or -1 for an empty slot; it is -1 wherever q // 4 + o - 1 lies outside 0 to 7. In every draw some device receives 12 filled slots from every device of its own group and of the two groups beside it. `recv_tgt`: entry [p, o, s, j] is the leaf of device p (counted from its first leaf) on which slot j from device (p // 4 + o - 1) * 4 + s acts; it is -1 exactly where that slot is empty or that device does not exist. `recv_type`: entry [p, o, s, j] selects the matrix of far_table for slot j from device (p // 4 + o - 1) * 4 + s to device p. `top_list`: row g names 4 different groups, none equal to g. `near_tgt`: counted from the device's first leaf. `near_src`: counted from 4 leaves before the device's first leaf; it lies within 4 leaves of the block's target leaf.
All inputs are finite; a program needn't handle non-finite values.
Results may differ from the reference program's by a relative error of at most 0.0003.
Values sent between devices are 32-bit elements; how exact they have to be, the bound alone decides.
A program may use at most 192 MiB of HBM per device.

```python
import jax
import jax.numpy as jnp
from jax import lax

PANEL = 128
RANK = 128
LEAF_DEV = 16
CAP = 12
NEAR_DEV = 64
HALO_L = 4
NTYPE = 32
K_TOP = 4
DEVS = 32
GROUPS = 8
NLEAVES = 512
PANELS = 65536
COLS = 128
N_SUB = 4


def far_plan(key):
    base = jax.random.fold_in(key, 17)
    fill_key, roll_key, full_key, source_key, target_key, kind_key = jax.random.split(base, 6)
    fill_share = jax.random.randint(fill_key, (DEVS,), 25, 76)
    roll_value = jax.random.randint(roll_key, (DEVS, 3, N_SUB, CAP), 0, 100)
    full_dest = jax.random.randint(full_key, (), N_SUB, DEVS - N_SUB)
    sender_ids = jnp.arange(DEVS, dtype=jnp.int32)[:, None, None, None]
    offsets = jnp.arange(3, dtype=jnp.int32)[None, :, None, None]
    subs = jnp.arange(N_SUB, dtype=jnp.int32)[None, None, :, None]
    receiver_group = sender_ids // N_SUB + offsets - 1
    receiver_valid = (receiver_group >= 0) & (receiver_group < GROUPS)
    receiver = jnp.clip(receiver_group, 0, GROUPS - 1) * N_SUB + subs
    used_slot = ((roll_value < fill_share[receiver]) | (receiver == full_dest)) & receiver_valid
    source_leaf = jax.random.randint(source_key, (DEVS, 3, N_SUB, CAP), 0, LEAF_DEV)
    target_leaf = jax.random.randint(target_key, (DEVS, 3, N_SUB, CAP), 0, LEAF_DEV)
    kind_ids = jax.random.randint(kind_key, (DEVS, 3, N_SUB, CAP), 0, NTYPE)
    return (used_slot, source_leaf, target_leaf, kind_ids)


def receiver_view(values):
    receivers = jnp.arange(DEVS, dtype=jnp.int32)
    group = receivers // N_SUB
    sub_index = receivers % N_SUB
    offsets = jnp.arange(3, dtype=jnp.int32)
    sender_groups = group[:, None] + offsets[None, :] - 1
    valid = (sender_groups >= 0) & (sender_groups < GROUPS)
    senders = jnp.clip(sender_groups, 0, GROUPS - 1)[:, :, None] * N_SUB + jnp.arange(N_SUB, dtype=jnp.int32)[None, None, :]
    back = jnp.broadcast_to((2 - offsets)[None, :, None], (DEVS, 3, N_SUB))
    subs = jnp.broadcast_to(sub_index[:, None, None], (DEVS, 3, N_SUB))
    return (values[senders, back, subs], jnp.broadcast_to(valid[:, :, None, None], (DEVS, 3, N_SUB, CAP)))


def draw_send_src(key, part):
    used_slot, source_leaf, target_leaf, kind_ids = far_plan(key)
    return jnp.where(used_slot, source_leaf, -1).astype(jnp.int32)


def draw_recv_tgt(key, part):
    used_slot, source_leaf, target_leaf, kind_ids = far_plan(key)
    used_view, valid = receiver_view(used_slot)
    target_view, valid = receiver_view(target_leaf)
    return jnp.where(used_view & valid, target_view, -1).astype(jnp.int32)


def draw_recv_type(key, part):
    used_slot, source_leaf, target_leaf, kind_ids = far_plan(key)
    kind_view, valid = receiver_view(kind_ids)
    return kind_view.astype(jnp.int32)


def near_plan(key):
    base = jax.random.fold_in(key, 29)
    target_key, offset_key = jax.random.split(base, 2)
    target_leaf = jax.random.randint(target_key, (DEVS, NEAR_DEV), 0, LEAF_DEV)
    offsets = jax.random.randint(offset_key, (DEVS, NEAR_DEV), -HALO_L, HALO_L + 1)
    return (target_leaf, target_leaf + HALO_L + offsets)


def draw_near_tgt(key, part):
    target_leaf, source_leaf = near_plan(key)
    return target_leaf.astype(jnp.int32)


def draw_near_src(key, part):
    target_leaf, source_leaf = near_plan(key)
    return source_leaf.astype(jnp.int32)


def draw_top_list(key, part):
    base = jax.random.fold_in(key, 41)
    scores = jax.random.randint(base, (GROUPS, GROUPS), 0, 4096) * GROUPS + jnp.arange(GROUPS, dtype=jnp.int32)[None, :]
    diagonal = jnp.arange(GROUPS, dtype=jnp.int32)[:, None] == jnp.arange(GROUPS, dtype=jnp.int32)[None, :]
    scores = jnp.where(diagonal, 2 ** 30, scores)
    ordering = jnp.argsort(scores, axis=1)
    return ordering[:, :K_TOP].astype(jnp.int32)


def place_ends(array, key, smallest, largest):
    longest = array.shape.index(max(array.shape))
    spots = []
    for shift in (0, 1):
        where = [jax.random.randint(jax.random.fold_in(key, axis), (), 0, length) for axis, length in enumerate(array.shape)]
        where[longest] = (where[longest] + shift) % array.shape[longest]
        spots.append(tuple(where))
    return array.at[spots[0]].set(smallest).at[spots[1]].set(largest)


def shard_levels(stream_key, extent, cuts, smallest, top_value):
    level, own = 1.0, jax.random.fold_in(stream_key, 6)
    for axis_at, parts in cuts:
        steps = jnp.exp(jax.random.uniform(jax.random.fold_in(own, axis_at), (parts,), jnp.float32, smallest / len(cuts), top_value / len(cuts)))
        level = level * jnp.repeat(steps, extent[axis_at] // parts).reshape([-1 if axis == axis_at else 1 for axis in range(len(extent))])
    return level


def scatter_about(own_key, extent, scale, bound, shards=(), kind=jnp.bfloat16):
    factor_of = shard_levels(own_key, extent, shards, -0.22, 0.18) if shards else 1.0
    entries = jax.random.normal(own_key, extent, jnp.float32) * scale * factor_of
    return jnp.minimum(jnp.maximum(entries, -bound), bound).astype(kind)


def setup_inputs(seed: int = 0) -> dict:
    key_of = jax.random.split(jax.random.key(seed), 15)
    return {
        "currents": scatter_about(key_of[0], (PANELS, COLS), 1.0, 6.0, ((0, 32),), jnp.float32),
        "leaf_basis": scatter_about(key_of[1], (NLEAVES, PANEL, RANK), PANEL ** -0.5, 0.5, ((0, 32),), jnp.float32),
        "leaf_rank": place_ends(jax.random.randint(key_of[2], (NLEAVES,), RANK // 2, RANK + 1), jax.random.fold_in(key_of[2], 1), RANK // 2, RANK).astype(jnp.int32),
        "leaf_transfer": scatter_about(key_of[3], (NLEAVES, RANK, RANK), (4 * RANK) ** -0.5, 0.25, ((0, 32),), jnp.float32),
        "top_transfer": scatter_about(key_of[4], (GROUPS, N_SUB, RANK, RANK), (2 * RANK) ** -0.5, 0.375, ((0, 8), (3, 4)), jnp.float32),
        "far_table": scatter_about(key_of[5], (NTYPE, 2, RANK, RANK), (2 * RANK * 3 * N_SUB * CAP // LEAF_DEV) ** -0.5, 0.125, (), jnp.float32),
        "send_src": draw_send_src(jax.random.fold_in(key_of[14], 71), 0),
        "recv_tgt": draw_recv_tgt(jax.random.fold_in(key_of[14], 71), 0),
        "recv_type": draw_recv_type(jax.random.fold_in(key_of[14], 71), 0),
        "top_coupling": scatter_about(key_of[9], (GROUPS, K_TOP, 2, RANK, RANK), (2 * RANK * K_TOP) ** -0.5, 0.1875, ((0, 8), (3, 4)), jnp.float32),
        "top_list": draw_top_list(jax.random.fold_in(key_of[14], 71), 0),
        "near_blocks": scatter_about(key_of[11], (DEVS * NEAR_DEV, 2, PANEL, PANEL), (2 * PANEL * NEAR_DEV // LEAF_DEV) ** -0.5, 0.1875, ((0, 32),), jnp.float32),
        "near_tgt": draw_near_tgt(jax.random.fold_in(key_of[14], 71), 0),
        "near_src": draw_near_src(jax.random.fold_in(key_of[14], 71), 0),
    }


exact_precision = lax.Precision.HIGHEST


def rotate(values):
    middle = values.shape[-1] // 2
    return jnp.concatenate([-values[..., middle:], values[..., :middle]], axis=-1)


def far_device(device, leaf_coef, send_src, recv_tgt, recv_type, far_table):
    group = device // N_SUB
    sub_index = device % N_SUB
    offsets = jnp.arange(3, dtype=jnp.int32)
    sender_groups = group + offsets - 1
    valid = (sender_groups >= 0) & (sender_groups < GROUPS)
    senders = jnp.clip(sender_groups, 0, GROUPS - 1)[:, None] * N_SUB + jnp.arange(N_SUB, dtype=jnp.int32)[None, :]
    back = jnp.broadcast_to((2 - offsets)[:, None], (3, N_SUB))
    sources = send_src[senders, back, sub_index]
    sources = jnp.where(valid[:, None, None], sources, -1)
    leaf_ids = senders[:, :, None] * LEAF_DEV + jnp.maximum(sources, 0)
    present = (sources >= 0).astype(jnp.float32)
    gathered = leaf_coef[leaf_ids] * present[:, :, :, None, None]
    slot_count = 3 * N_SUB * CAP
    gathered = gathered.reshape(slot_count, RANK, gathered.shape[-1])
    kind_ids = lax.dynamic_index_in_dim(recv_type, device, axis=0, keepdims=False).reshape(slot_count)
    targets = lax.dynamic_index_in_dim(recv_tgt, device, axis=0, keepdims=False).reshape(slot_count)
    matrices = far_table[kind_ids]
    operator_product = jnp.einsum("sab,sbc->sac", matrices[:, 0], gathered, precision=exact_precision)
    operator_product = operator_product + jnp.einsum("sab,sbc->sac", matrices[:, 1], rotate(gathered), precision=exact_precision)
    selector_matrix = (targets[:, None] == jnp.arange(LEAF_DEV, dtype=jnp.int32)[None, :]).astype(jnp.float32)
    return jnp.einsum("iv,ibg->vbg", selector_matrix, operator_product, precision=exact_precision)


def near_device(device, leaf_currents, blocks, near_tgt, near_src):
    extended = lax.dynamic_index_in_dim(near_src, device, axis=0, keepdims=False)
    leaf_ids = device * LEAF_DEV + extended - HALO_L
    inside_grid = ((leaf_ids >= 0) & (leaf_ids < NLEAVES)).astype(jnp.float32)
    sources = leaf_currents[jnp.clip(leaf_ids, 0, NLEAVES - 1)] * inside_grid[:, None, None]
    own_blocks = lax.dynamic_index_in_dim(blocks, device, axis=0, keepdims=False)
    operator_product = jnp.einsum("nab,nbc->nac", own_blocks[:, 0], sources, precision=exact_precision)
    operator_product = operator_product + jnp.einsum("nab,nbc->nac", own_blocks[:, 1], rotate(sources), precision=exact_precision)
    targets = lax.dynamic_index_in_dim(near_tgt, device, axis=0, keepdims=False)
    selector_matrix = (targets[:, None] == jnp.arange(LEAF_DEV, dtype=jnp.int32)[None, :]).astype(jnp.float32)
    return jnp.einsum("if,ivo->fvo", selector_matrix, operator_product, precision=exact_precision)


def reference(currents, leaf_basis, leaf_rank, leaf_transfer, top_transfer, far_table, send_src, recv_tgt, recv_type, top_coupling, top_list, near_blocks, near_tgt, near_src):
    columns = currents.shape[1]
    rank_mask = (jnp.arange(RANK, dtype=jnp.int32)[None, :] < leaf_rank[:, None]).astype(jnp.float32)
    masked_basis = leaf_basis * rank_mask[:, None, :]
    leaf_currents = currents.reshape(NLEAVES, PANEL, columns)
    leaf_coef = jnp.einsum("lpr,lpc->lrc", masked_basis, leaf_currents, precision=exact_precision)
    lifted = jnp.einsum("lab,lac->lbc", leaf_transfer, leaf_coef, precision=exact_precision)
    mid_coef = lifted.reshape(DEVS, LEAF_DEV, RANK, columns).sum(axis=1)
    grouped = mid_coef.reshape(GROUPS, N_SUB, RANK, columns)
    top_coef = jnp.einsum("gsab,gsac->gbc", top_transfer, grouped, precision=exact_precision)
    partners = top_coef[top_list]
    top_field = jnp.einsum("gkab,gkbc->gac", top_coupling[:, :, 0], partners, precision=exact_precision)
    top_field = top_field + jnp.einsum("gkab,gkbc->gac", top_coupling[:, :, 1], rotate(partners), precision=exact_precision)
    mid_field = jnp.einsum("gsab,gbc->gsac", top_transfer, top_field, precision=exact_precision).reshape(DEVS, RANK, columns)
    down_field = jnp.einsum("lab,lbc->lac", leaf_transfer, jnp.repeat(mid_field, LEAF_DEV, axis=0), precision=exact_precision)
    far_field = lax.map(lambda device: far_device(device, leaf_coef, send_src, recv_tgt, recv_type, far_table), jnp.arange(DEVS, dtype=jnp.int32))
    leaf_field = far_field.reshape(NLEAVES, RANK, columns) + down_field
    far_part = jnp.einsum("lpr,lrc->lpc", masked_basis, leaf_field, precision=exact_precision)
    blocks = near_blocks.reshape(DEVS, NEAR_DEV, 2, PANEL, PANEL)
    near_field_share = lax.map(lambda device: near_device(device, leaf_currents, blocks, near_tgt, near_src), jnp.arange(DEVS, dtype=jnp.int32))
    near_field_share = near_field_share.reshape(NLEAVES, PANEL, columns)
    return (far_part + near_field_share).reshape(PANELS, columns)
```

```python
import functools

import jax
import jax.numpy as jnp
from jax import lax
from jax.experimental import pallas as pl
from jax.experimental.pallas import tpu as pltpu
from jax.sharding import PartitionSpec as P

HALO_L = 4
F32 = jnp.float32
BF16 = jnp.bfloat16
NN = (((1,), (0,)), ((), ()))
TN = (((0,), (0,)), ((), ()))


SMEM = pl.BlockSpec(memory_space=pltpu.SMEM)
VMEM = pl.BlockSpec(memory_space=pltpu.VMEM)
MESH = pl.DeviceIdType.MESH


def shifted(value, axis, by):
    length = lax.axis_size(axis)
    pairs = [(i, i + by) for i in range(length) if 0 <= i + by < length]
    return lax.ppermute(value, axis, pairs)


def split(x):
    high = x.astype(BF16)
    return high, (x - high.astype(F32)).astype(BF16)


def dot(a, b, dims=NN):
    return lax.dot_general(a, b, dims, preferred_element_type=F32)


def dot3(a, b, dims=NN):
    ah, al = split(a)
    bh, bl = split(b)
    return dot(ah, bh, dims) + (dot(ah, bl, dims) + dot(al, bh, dims))


def rotated(c):
    half = c.shape[-1] // 2
    lane = lax.broadcasted_iota(jnp.int32, c.shape, c.ndim - 1)
    turned_c = pltpu.roll(c, half, c.ndim - 1)
    return jnp.where(lane < half, -turned_c, turned_c)


def lay_out(store, at, c):
    rows, cols = c.shape
    high, low = split(c)
    rhigh, rlow = split(rotated(c))
    store[at, :rows, :cols] = high
    store[at, :rows, cols:] = low
    store[at, rows:, :cols] = rhigh
    store[at, rows:, cols:] = rlow


def applied(mh, ml, b):
    cols = b.shape[1] // 2
    p = dot(mh, b)
    return p[:, :cols] + (p[:, cols:] + dot(ml, b[:, :cols]))


def masked(basis, rank):
    lane = lax.broadcasted_iota(jnp.int32, basis.shape, 1)
    return jnp.where(lane < rank, basis, 0.0)


def params(mb=48):
    return pltpu.CompilerParams(vmem_limit_bytes=mb * 1024 * 1024)


def cost(flops, nbytes):
    return pl.CostEstimate(flops=int(flops), bytes_accessed=int(nbytes), transcendentals=0)


def up_kernel(per, rank, cur, basis, transfer, coef, mid):
    step = pl.program_id(0)

    @pl.when(step == 0)
    def _():
        mid[...] = jnp.zeros_like(mid)

    total = mid[...]
    for i in range(per):
        c = dot3(masked(basis[i], rank[step * per + i]), cur[i], TN)
        coef[i] = c
        total += dot3(transfer[i], c, TN)
    mid[...] = total


def up(rank, cur, basis, transfer):
    leaves, panel, width = basis.shape
    cols = cur.shape[2]
    per = 4
    block = lambda a: pl.BlockSpec((per,) + a.shape[1:], lambda i: (i, 0, 0))
    return pl.pallas_call(
        functools.partial(up_kernel, per),
        grid=(leaves // per,),
        in_specs=[SMEM, block(cur), block(basis), block(transfer)],
        out_specs=[
            pl.BlockSpec((per, width, cols), lambda i: (i, 0, 0)),
            pl.BlockSpec((width, cols), lambda i: (0, 0)),
        ],
        out_shape=[
            jax.ShapeDtypeStruct((leaves, width, cols), F32),
            jax.ShapeDtypeStruct((width, cols), F32),
        ],
        compiler_params=params(),
        cost_estimate=cost(leaves * 12 * panel * width * cols, 16 * leaves * panel * width),
        name="up",
    )(rank, cur, basis, transfer)


def table_kernel(table, high, low):
    for i in range(table.shape[0]):
        h0, l0 = split(table[i, 0])
        h1, l1 = split(table[i, 1])
        w = h0.shape[1]
        high[i, :, :w] = h0
        high[i, :, w:] = h1
        low[i, :, :w] = l0
        low[i, :, w:] = l1


def split_table(table):
    kinds, two, a, b = table.shape
    per = 8 if kinds % 8 == 0 else 1
    out = pl.BlockSpec((per, a, 2 * b), lambda i: (i, 0, 0))
    return pl.pallas_call(
        table_kernel,
        grid=(kinds // per,),
        in_specs=[pl.BlockSpec((per, 2, a, b), lambda i: (i, 0, 0, 0))],
        out_specs=[out, out],
        out_shape=[jax.ShapeDtypeStruct((kinds, a, 2 * b), BF16)] * 2,
        compiler_params=params(),
        cost_estimate=cost(kinds * a * b * 20, kinds * a * b * 16),
        name="table",
    )(table)


def near_kernel(per, tgt, src, below, cur, above, blocks, out, laid):
    step = pl.program_id(0)

    @pl.when(step == 0)
    def _():
        out[...] = jnp.zeros_like(out)
        base = 0
        for part in (below, cur, above):
            @pl.loop(0, part.shape[0], unroll=2)
            def _(l, part=part, base=base):
                lay_out(laid, base + l, part[l])

            base += part.shape[0]

    results = []
    for u in range(per):
        h0, l0 = split(blocks[u, 0])
        h1, l1 = split(blocks[u, 1])
        b = laid[src[step * per + u]]
        results.append(
            applied(
                jnp.concatenate([h0, h1], axis=1), jnp.concatenate([l0, l1], axis=1), b
            )
        )
    for u in range(per):
        out[tgt[step * per + u]] += results[u]


def near(tgt, src, below, cur, above, blocks):
    count, two, a, b = blocks.shape
    leaves, panel, cols = cur.shape
    per = 4 if count % 4 == 0 else 1
    total = leaves + below.shape[0] + above.shape[0]
    whole = lambda x: pl.BlockSpec(x.shape, lambda i: (0,) * x.ndim)
    return pl.pallas_call(
        functools.partial(near_kernel, per),
        grid=(count // per,),
        in_specs=[
            SMEM,
            SMEM,
            whole(below),
            whole(cur),
            whole(above),
            pl.BlockSpec((per, two, a, b), lambda i: (i, 0, 0, 0)),
        ],
        out_specs=pl.BlockSpec((leaves, a, cols), lambda i: (0, 0, 0)),
        out_shape=jax.ShapeDtypeStruct((leaves, a, cols), F32),
        scratch_shapes=[pltpu.VMEM((total, 2 * b, 2 * cols), BF16)],
        compiler_params=params(),
        cost_estimate=cost(count * 12 * a * b * cols, count * 8 * a * b),
        name="near",
    )(tgt, src, below, cur, above, blocks)


CHUNKS = 4
FAR, SECOND, END, OWN = range(4)


def ordered(tgt, src, kind, leaves):
    count = tgt.shape[-1]
    spot = jnp.arange(count, dtype=jnp.int32)
    key = jnp.where(tgt < 0, leaves, tgt)
    src = jnp.where(tgt < 0, leaves, src)
    mine, other = key[:, :, None], key[:, None, :]
    before = (other < mine) | ((other == mine) & (spot[None, None, :] < spot[None, :, None]))
    place = jnp.sum(before.astype(jnp.int32), axis=2)
    hot = place[:, None, :] == spot[None, :, None]
    pick = lambda x: jnp.sum(jnp.where(hot, x[:, None, :], 0), axis=2)
    key = pick(key)
    keep = jnp.concatenate(
        [jnp.zeros_like(key[:, :1]), (key[:, 1:] == key[:, :-1]).astype(jnp.int32)], axis=1
    )
    leaf = jnp.arange(leaves, dtype=jnp.int32)
    last = jnp.max(jnp.where(key[:, None, :] == leaf[None, :, None], spot, -1), axis=2)
    return jnp.stack([pick(src), pick(kind), keep]), last


def fields_kernel(
    unroll,
    slots,
    last,
    partner,
    rank,
    own,
    prev,
    nxt,
    ext,
    high,
    low,
    basis,
    transfer,
    near_part,
    mid,
    top_transfer,
    coupling,
    out,
    laid,
    laid_ext,
    ext_in,
    runs,
    part,
    from_end,
    from_other,
    mids,
    top_own,
    tops,
    shares,
    shares_in,
    down,
    out_sem,
    end_sem,
    other_sem,
    back_sem,
    ext_sem,
    mid_sem,
    top_sem,
    all_sem,
    down_sem,
):
    n = lax.axis_size("sub")
    groups = lax.axis_size("leaf")
    me = lax.axis_index("sub")
    group = lax.axis_index("leaf")
    leaves = own.shape[0]
    count = slots.shape[2]
    per = leaves // CHUNKS
    share = top_own.shape[0] // n
    low_side = me < n // 2
    is_end = (me == 0) | (me == n - 1)
    is_inner = (me != 0) & (me != n - 1)
    end = jnp.where(low_side, 0, n - 1)
    inner = jnp.where(low_side, 1, n - 2)
    other = n - 1 - inner

    barrier = pltpu.get_barrier_semaphore()
    for d in range(1, n):
        pl.semaphore_signal(
            barrier, inc=1, device_id=(group, lax.rem(me + d, n)), device_id_type=MESH
        )
    for d in range(1, groups):
        pl.semaphore_signal(
            barrier, inc=1, device_id=(lax.rem(group + d, groups), me), device_id_type=MESH
        )

    @pl.loop(0, leaves, unroll=2)
    def _(l):
        lay_out(laid, l, prev[l])
        lay_out(laid, leaves + l, own[l])
        lay_out(laid, 2 * leaves + l, nxt[l])

    pl.semaphore_wait(barrier, n + groups - 2)

    def remote(source, target, send, recv, device):
        return pltpu.make_async_remote_copy(
            src_ref=source,
            dst_ref=target,
            send_sem=send,
            recv_sem=recv,
            device_id=device,
            device_id_type=MESH,
        )

    def ext_copy(side):
        there = jnp.clip(group + (1 if side == 0 else -1), 0, groups - 1)
        return remote(ext, ext_in.at[side], ext_sem.at[0, side], ext_sem.at[1, side], (there, me))

    sends_ext = [is_inner & (group + 1 < groups), is_inner & (group > 0)]
    takes_ext = [is_inner & (group > 0), is_inner & (group + 1 < groups)]
    for side in range(2):
        @pl.when(sends_ext[side])
        def _(side=side):
            ext_copy(side).start()

    def mid_copy(d):
        return remote(
            mid, mids.at[me], mid_sem.at[0, d - 1], mid_sem.at[1, d - 1], (group, lax.rem(me + d, n))
        )

    for d in range(1, n):
        mid_copy(d).start()

    def compute(at, store, role, add=False):
        def step(i, acc):
            results = []
            for u in range(unroll):
                j = i * unroll + u
                k = slots[1, at, j]
                results.append(applied(high[k], low[k], store[slots[0, at, j]]))
            for u in range(unroll):
                j = i * unroll + u
                acc = acc * slots[2, at, j].astype(F32) + results[u]
                runs[j] = acc
            return acc

        lax.fori_loop(0, count // unroll, step, jnp.zeros(runs.shape[1:], F32))

        @pl.loop(0, leaves, unroll=2)
        def _(l):
            j = last[at, l]
            value = runs[jnp.maximum(j, 0)] * jnp.where(j >= 0, 1.0, 0.0)
            part[role, l] = part[role, l] + value if add else value

    def chunk(c):
        return pl.ds(c * per, per)

    def end_copy(role, c):
        return remote(
            part.at[role, chunk(c)],
            from_end.at[role, chunk(c)],
            out_sem.at[role, c],
            end_sem.at[role, c],
            (group, inner),
        )

    def other_copy(role, c):
        return remote(
            part.at[role, chunk(c)],
            from_other.at[role, chunk(c)],
            out_sem.at[role, c],
            other_sem.at[role, c],
            (group, other),
        )

    def back_copy(c):
        return remote(
            part.at[END, chunk(c)],
            from_other.at[1, chunk(c)],
            back_sem.at[c],
            other_sem.at[1, c],
            (group, end),
        )

    def relay(role, c):
        @pl.when(is_inner)
        def _():
            end_copy(role, c).wait_recv()
            part[role, chunk(c)] += from_end[role, chunk(c)]
            other_copy(role, c).start()

    def relay_back(c):
        @pl.when(is_inner)
        def _():
            other_copy(0, c).wait_recv()
            part[END, chunk(c)] += from_other[0, chunk(c)]
            back_copy(c).start()

    compute(n - 1 - end, laid, FAR)

    @pl.when(is_end)
    def _():
        for c in range(CHUNKS):
            end_copy(FAR, c).start()

    compute(other, laid, SECOND)

    @pl.when(is_end)
    def _():
        for c in range(CHUNKS):
            end_copy(SECOND, c).start()

    mids[me] = mid[...]
    for d in range(1, n):
        mid_copy(d).wait_recv()
    total = dot3(top_transfer[0], mids[0], TN)
    for s in range(1, n):
        total += dot3(top_transfer[s], mids[s], TN)
    mine = pl.ds(pl.multiple_of(me * share, share), share)
    top_own[mine, :] = total

    def top_copy(d):
        return remote(
            top_own.at[mine],
            top_own.at[mine],
            top_sem.at[0, d - 1],
            top_sem.at[1, d - 1],
            (group, lax.rem(me + d, n)),
        )

    for d in range(1, n):
        top_copy(d).start()

    @pl.when(is_inner)
    def _():
        compute(end, laid, END)

    relay(FAR, 0)
    compute(me, laid, OWN)
    relay(FAR, 1)

    def all_copy(d):
        return remote(
            top_own,
            tops.at[group],
            all_sem.at[0, d - 1],
            all_sem.at[1, d - 1],
            (lax.rem(group + d, groups), me),
        )

    for d in range(1, n):
        top_copy(d).wait_recv()
    for d in range(1, groups):
        all_copy(d).start()
    tops[group] = top_own[...]
    relay_back(0)
    relay(FAR, 2)
    relay_back(1)

    for d in range(1, groups):
        all_copy(d).wait_recv()
    field = jnp.zeros((share, mid.shape[1]), F32)
    for k in range(partner.shape[0]):
        p = tops[partner[k]]
        field += dot3(coupling[k, 0], p) + dot3(coupling[k, 1], rotated(p))
    for s in range(n):
        shares[s] = dot3(top_transfer[s], field)

    def down_copy(d):
        there = lax.rem(me + d, n)
        return remote(
            shares.at[there],
            shares_in.at[me],
            down_sem.at[0, d - 1],
            down_sem.at[1, d - 1],
            (group, there),
        )

    for d in range(1, n):
        down_copy(d).start()

    for side in range(2):
        @pl.when(takes_ext[side])
        def _(side=side):
            ext_copy(side).wait_recv()

            @pl.loop(0, leaves, unroll=2)
            def _(l):
                lay_out(laid_ext, (0 if side == 0 else 2 * leaves) + l, ext_in[side, l])

    @pl.when(is_inner)
    def _():
        @pl.loop(0, leaves, unroll=2)
        def _(l):
            lay_out(laid_ext, leaves + l, ext[l])

        compute(n, laid_ext, OWN, add=True)

    relay(FAR, 3)
    relay_back(2)

    shares_in[me] = shares[me]
    for d in range(1, n):
        down_copy(d).wait_recv()
    total = shares_in[0]
    for s in range(1, n):
        total += shares_in[s]
    down[...] = total

    @pl.loop(0, leaves, unroll=2)
    def _(l):
        part[OWN, l] += dot3(transfer[l], down[...])

    def finish(c):
        other_copy(1, c).wait_recv()
        for i in range(per):
            l = c * per + i
            field = part[OWN, l] + from_other[1, l]
            out[l] = dot3(masked(basis[l], rank[l]), field) + near_part[l]

    relay(SECOND, 0)
    relay_back(3)
    relay(SECOND, 1)
    finish(0)
    relay(SECOND, 2)
    finish(1)
    relay(SECOND, 3)
    finish(2)
    finish(3)

    for side in range(2):
        @pl.when(sends_ext[side])
        def _(side=side):
            ext_copy(side).wait_send()
    for d in range(1, n):
        mid_copy(d).wait_send()
        top_copy(d).wait_send()
        down_copy(d).wait_send()
    for d in range(1, groups):
        all_copy(d).wait_send()
    for c in range(CHUNKS):
        end_copy(FAR, c).wait_send()
        end_copy(SECOND, c).wait_send()

        @pl.when(is_inner)
        def _(c=c):
            back_copy(c).wait_send()


def fields(slots, last, partner, rank, coefs, tables, own_parts, top_parts):
    own, prev, nxt, ext = coefs
    leaves, width, cols = own.shape
    count = slots.shape[2]
    n = lax.axis_size("sub")
    groups = lax.axis_size("leaf")
    unroll = max(u for u in range(1, 7) if count % u == 0)
    block = lambda *lead: pltpu.VMEM(lead + (width, cols), F32)
    dma = lambda *shape: pltpu.SemaphoreType.DMA(shape)
    operands = [*coefs, *tables, *own_parts, *top_parts]
    return pl.pallas_call(
        functools.partial(fields_kernel, unroll),
        in_specs=[SMEM] * 4 + [VMEM] * len(operands),
        out_specs=VMEM,
        out_shape=jax.ShapeDtypeStruct((leaves, width, cols), F32),
        scratch_shapes=[
            pltpu.VMEM((3 * leaves, 2 * width, 2 * cols), BF16),
            pltpu.VMEM((3 * leaves, 2 * width, 2 * cols), BF16),
            block(2, leaves),
            block(count),
            block(4, leaves),
            block(2, leaves),
            block(2, leaves),
            block(n),
            block(),
            block(groups),
            block(n),
            block(n),
            block(),
            dma(2, CHUNKS),
            dma(2, CHUNKS),
            dma(2, CHUNKS),
            dma(CHUNKS),
            dma(2, 2),
            dma(2, n - 1),
            dma(2, n - 1),
            dma(2, groups - 1),
            dma(2, n - 1),
        ],
        compiler_params=pltpu.CompilerParams(
            vmem_limit_bytes=60 * 1024 * 1024, collective_id=0, has_side_effects=True
        ),
        cost_estimate=cost(5 * count * 12 * width * width * cols, 12 * 2 ** 20),
        name="fields",
    )(slots, last, partner, rank, *operands)


def per_device(
    currents,
    leaf_basis,
    leaf_rank,
    leaf_transfer,
    top_transfer,
    far_table,
    send_src,
    recv_tgt,
    recv_type,
    top_coupling,
    top_list,
    near_blocks,
    near_tgt,
    near_src,
):
    leaves, panel, width = leaf_basis.shape
    cols = currents.shape[1]
    n = lax.axis_size("sub")
    me = lax.axis_index("sub")
    cur = currents.reshape(leaves, panel, cols)
    ends = [(0, 1), (n - 1, n - 2)]
    inner = jnp.where(me < n // 2, 1, n - 2)
    end = jnp.where(me < n // 2, 0, n - 1)

    below_rim = shifted(cur[leaves - HALO_L :], ("leaf", "sub"), 1)
    above_rim = shifted(cur[:HALO_L], ("leaf", "sub"), -1)
    recv = jnp.stack([recv_tgt[0], recv_type[0]])
    theirs = lax.all_to_all(jnp.moveaxis(recv, 2, 0), "sub", 0, 0)
    sources = send_src[0]
    sources = jnp.stack(
        [shifted(sources[2], "leaf", 1), sources[1] + leaves, shifted(sources[0], "leaf", -1) + 2 * leaves]
    )
    extra_src = lax.ppermute(lax.dynamic_index_in_dim(sources, inner, 1, False), "sub", ends)
    extra = lax.dynamic_index_in_dim(recv, end, 2, False)
    flat = lambda x: x.reshape(x.shape[0], -1)
    both = jnp.concatenate([theirs, extra[None]], axis=0)
    all_src = jnp.concatenate([jnp.moveaxis(sources, 1, 0), extra_src[None]], axis=0)
    slots, last = ordered(flat(both[:, 0]), flat(all_src), flat(both[:, 1]), leaves)

    coef, mid = up(leaf_rank, cur, leaf_basis, leaf_transfer)
    prev, nxt = shifted(coef, "leaf", 1), shifted(coef, "leaf", -1)
    ext = lax.ppermute(coef, "sub", ends)
    tables = split_table(far_table)
    near_part = near(near_tgt[0], near_src[0], below_rim, cur, above_rim, near_blocks)
    out = fields(
        slots,
        last,
        top_list[0],
        leaf_rank,
        [coef, prev, nxt, ext],
        tables,
        [leaf_basis, leaf_transfer, near_part],
        [mid, top_transfer[0], top_coupling[0]],
    )
    return out.reshape(leaves * panel, cols)


def solution(mesh):
    placed = (
        P(("leaf", "sub"), None),
        P(("leaf", "sub"), None, None),
        P(("leaf", "sub")),
        P(("leaf", "sub"), None, None),
        P("leaf", None, None, "sub"),
        P(),
        P(("leaf", "sub"), None, None, None),
        P(("leaf", "sub"), None, None, None),
        P(("leaf", "sub"), None, None, None),
        P("leaf", None, None, "sub", None),
        P("leaf", None),
        P(("leaf", "sub"), None, None, None),
        P(("leaf", "sub"), None),
        P(("leaf", "sub"), None),
    )
    return jax.shard_map(
        per_device, mesh=mesh, in_specs=placed, out_specs=P(("leaf", "sub"), None), check_vma=False
    )
```

```python
import functools

import jax
import jax.numpy as jnp
from jax import lax
from jax.experimental import pallas as pl
from jax.experimental.pallas import tpu as pltpu
from jax.sharding import PartitionSpec as P

HALO_L = 4
F32 = jnp.float32
BF16 = jnp.bfloat16
NN = (((1,), (0,)), ((), ()))
TN = (((0,), (0,)), ((), ()))


SMEM = pl.BlockSpec(memory_space=pltpu.SMEM)
VMEM = pl.BlockSpec(memory_space=pltpu.VMEM)
MESH = pl.DeviceIdType.MESH


def shifted(value, axis, by):
    length = lax.axis_size(axis)
    pairs = [(i, i + by) for i in range(length) if 0 <= i + by < length]
    return lax.ppermute(value, axis, pairs)


def split(x):
    high = x.astype(BF16)
    return high, (x - high.astype(F32)).astype(BF16)


def dot(a, b, dims=NN):
    return lax.dot_general(a, b, dims, preferred_element_type=F32)


def dot3(a, b, dims=NN):
    ah, al = split(a)
    bh, bl = split(b)
    return dot(ah, bh, dims) + (dot(ah, bl, dims) + dot(al, bh, dims))


def rotated(c):
    half = c.shape[-1] // 2
    lane = lax.broadcasted_iota(jnp.int32, c.shape, c.ndim - 1)
    turned_c = pltpu.roll(c, half, c.ndim - 1)
    return jnp.where(lane < half, -turned_c, turned_c)


def lay_out(store, at, c):
    rows, cols = c.shape
    high, low = split(c)
    rhigh, rlow = split(rotated(c))
    store[at, :rows, :cols] = high
    store[at, :rows, cols:] = low
    store[at, rows:, :cols] = rhigh
    store[at, rows:, cols:] = rlow


def applied(mh, ml, b):
    cols = b.shape[1] // 2
    p = dot(mh, b)
    return p[:, :cols] + (p[:, cols:] + dot(ml, b[:, :cols]))


def masked(basis, rank):
    lane = lax.broadcasted_iota(jnp.int32, basis.shape, 1)
    return jnp.where(lane < rank, basis, 0.0)


def params(mb=48):
    return pltpu.CompilerParams(vmem_limit_bytes=mb * 1024 * 1024)


def cost(flops, nbytes):
    return pl.CostEstimate(flops=int(flops), bytes_accessed=int(nbytes), transcendentals=0)


def up_kernel(per, rank, cur, basis, transfer, coef, mid):
    step = pl.program_id(0)

    @pl.when(step == 0)
    def _():
        mid[...] = jnp.zeros_like(mid)

    total = mid[...]
    for i in range(per):
        c = dot3(masked(basis[i], rank[step * per + i]), cur[i], TN)
        coef[i] = c
        total += dot3(transfer[i], c, TN)
    mid[...] = total


def up(rank, cur, basis, transfer):
    leaves, panel, width = basis.shape
    cols = cur.shape[2]
    per = 4
    block = lambda a: pl.BlockSpec((per,) + a.shape[1:], lambda i: (i, 0, 0))
    return pl.pallas_call(
        functools.partial(up_kernel, per),
        grid=(leaves // per,),
        in_specs=[SMEM, block(cur), block(basis), block(transfer)],
        out_specs=[
            pl.BlockSpec((per, width, cols), lambda i: (i, 0, 0)),
            pl.BlockSpec((width, cols), lambda i: (0, 0)),
        ],
        out_shape=[
            jax.ShapeDtypeStruct((leaves, width, cols), F32),
            jax.ShapeDtypeStruct((width, cols), F32),
        ],
        compiler_params=params(),
        cost_estimate=cost(leaves * 12 * panel * width * cols, 16 * leaves * panel * width),
        name="up",
    )(rank, cur, basis, transfer)


def table_kernel(table, high, low):
    for i in range(table.shape[0]):
        h0, l0 = split(table[i, 0])
        h1, l1 = split(table[i, 1])
        w = h0.shape[1]
        high[i, :, :w] = h0
        high[i, :, w:] = h1
        low[i, :, :w] = l0
        low[i, :, w:] = l1


def split_table(table):
    kinds, two, a, b = table.shape
    per = 8 if kinds % 8 == 0 else 1
    out = pl.BlockSpec((per, a, 2 * b), lambda i: (i, 0, 0))
    return pl.pallas_call(
        table_kernel,
        grid=(kinds // per,),
        in_specs=[pl.BlockSpec((per, 2, a, b), lambda i: (i, 0, 0, 0))],
        out_specs=[out, out],
        out_shape=[jax.ShapeDtypeStruct((kinds, a, 2 * b), BF16)] * 2,
        compiler_params=params(),
        cost_estimate=cost(kinds * a * b * 20, kinds * a * b * 16),
        name="table",
    )(table)


def near_kernel(per, tgt, src, below, cur, above, blocks, out, laid):
    step = pl.program_id(0)

    @pl.when(step == 0)
    def _():
        out[...] = jnp.zeros_like(out)
        base = 0
        for part in (below, cur, above):
            @pl.loop(0, part.shape[0], unroll=2)
            def _(l, part=part, base=base):
                lay_out(laid, base + l, part[l])

            base += part.shape[0]

    results = []
    for u in range(per):
        h0, l0 = split(blocks[u, 0])
        h1, l1 = split(blocks[u, 1])
        b = laid[src[step * per + u]]
        results.append(
            applied(
                jnp.concatenate([h0, h1], axis=1), jnp.concatenate([l0, l1], axis=1), b
            )
        )
    for u in range(per):
        out[tgt[step * per + u]] += results[u]


def near(tgt, src, below, cur, above, blocks):
    count, two, a, b = blocks.shape
    leaves, panel, cols = cur.shape
    per = 4 if count % 4 == 0 else 1
    total = leaves + below.shape[0] + above.shape[0]
    whole = lambda x: pl.BlockSpec(x.shape, lambda i: (0,) * x.ndim)
    return pl.pallas_call(
        functools.partial(near_kernel, per),
        grid=(count // per,),
        in_specs=[
            SMEM,
            SMEM,
            whole(below),
            whole(cur),
            whole(above),
            pl.BlockSpec((per, two, a, b), lambda i: (i, 0, 0, 0)),
        ],
        out_specs=pl.BlockSpec((leaves, a, cols), lambda i: (0, 0, 0)),
        out_shape=jax.ShapeDtypeStruct((leaves, a, cols), F32),
        scratch_shapes=[pltpu.VMEM((total, 2 * b, 2 * cols), BF16)],
        compiler_params=params(),
        cost_estimate=cost(count * 12 * a * b * cols, count * 8 * a * b),
        name="near",
    )(tgt, src, below, cur, above, blocks)


CHUNKS = 8
FLIGHT = 2
FAR, SECOND, END, OWN = range(4)


def ordered(tgt, src, kind, leaves):
    count = tgt.shape[-1]
    spot = jnp.arange(count, dtype=jnp.int32)
    key = jnp.where(tgt < 0, leaves, tgt)
    src = jnp.where(tgt < 0, leaves, src)
    mine, other = key[:, :, None], key[:, None, :]
    before = (other < mine) | ((other == mine) & (spot[None, None, :] < spot[None, :, None]))
    place = jnp.sum(before.astype(jnp.int32), axis=2)
    hot = place[:, None, :] == spot[None, :, None]
    pick = lambda x: jnp.sum(jnp.where(hot, x[:, None, :], 0), axis=2)
    key = pick(key)
    keep = jnp.concatenate(
        [jnp.zeros_like(key[:, :1]), (key[:, 1:] == key[:, :-1]).astype(jnp.int32)], axis=1
    )
    leaf = jnp.arange(leaves, dtype=jnp.int32)
    last = jnp.max(jnp.where(key[:, None, :] == leaf[None, :, None], spot, -1), axis=2)
    return jnp.stack([pick(src), pick(kind), keep]), last


def fields_kernel(
    unroll,
    slots,
    last,
    partner,
    rank,
    own,
    prev,
    nxt,
    ext,
    high,
    low,
    basis,
    transfer,
    near_part,
    mid,
    top_transfer,
    coupling,
    out,
    laid,
    laid_ext,
    ext_in,
    runs,
    part,
    from_end,
    from_other,
    mids,
    top_own,
    tops,
    shares,
    shares_in,
    down,
    out_sem,
    end_sem,
    other_sem,
    back_sem,
    ext_sem,
    mid_sem,
    top_sem,
    all_sem,
    down_sem,
):
    n = lax.axis_size("sub")
    groups = lax.axis_size("leaf")
    me = lax.axis_index("sub")
    group = lax.axis_index("leaf")
    leaves = own.shape[0]
    count = slots.shape[2]
    per = leaves // CHUNKS
    share = top_own.shape[0] // n
    low_side = me < n // 2
    is_end = (me == 0) | (me == n - 1)
    is_inner = (me != 0) & (me != n - 1)
    end = jnp.where(low_side, 0, n - 1)
    inner = jnp.where(low_side, 1, n - 2)
    other = n - 1 - inner

    barrier = pltpu.get_barrier_semaphore()
    for d in range(1, n):
        pl.semaphore_signal(
            barrier, inc=1, device_id=(group, lax.rem(me + d, n)), device_id_type=MESH
        )
    for d in range(1, groups):
        pl.semaphore_signal(
            barrier, inc=1, device_id=(lax.rem(group + d, groups), me), device_id_type=MESH
        )

    @pl.loop(0, leaves, unroll=2)
    def _(l):
        lay_out(laid, l, prev[l])
        lay_out(laid, leaves + l, own[l])
        lay_out(laid, 2 * leaves + l, nxt[l])

    pl.semaphore_wait(barrier, n + groups - 2)

    def remote(source, target, send, recv, device):
        return pltpu.make_async_remote_copy(
            src_ref=source,
            dst_ref=target,
            send_sem=send,
            recv_sem=recv,
            device_id=device,
            device_id_type=MESH,
        )

    def ext_copy(side):
        there = jnp.clip(group + (1 if side == 0 else -1), 0, groups - 1)
        return remote(ext, ext_in.at[side], ext_sem.at[0, side], ext_sem.at[1, side], (there, me))

    sends_ext = [is_inner & (group + 1 < groups), is_inner & (group > 0)]
    takes_ext = [is_inner & (group > 0), is_inner & (group + 1 < groups)]
    for side in range(2):
        @pl.when(sends_ext[side])
        def _(side=side):
            ext_copy(side).start()

    def mid_copy(d):
        return remote(
            mid, mids.at[me], mid_sem.at[0, d - 1], mid_sem.at[1, d - 1], (group, lax.rem(me + d, n))
        )

    for d in range(1, n):
        mid_copy(d).start()

    def compute(at, store, role, add=False):
        def step(i, acc):
            results = []
            for u in range(unroll):
                j = i * unroll + u
                k = slots[1, at, j]
                results.append(applied(high[k], low[k], store[slots[0, at, j]]))
            for u in range(unroll):
                j = i * unroll + u
                acc = acc * slots[2, at, j].astype(F32) + results[u]
                runs[j] = acc
            return acc

        lax.fori_loop(0, count // unroll, step, jnp.zeros(runs.shape[1:], F32))

        @pl.loop(0, leaves, unroll=2)
        def _(l):
            j = last[at, l]
            value = runs[jnp.maximum(j, 0)] * jnp.where(j >= 0, 1.0, 0.0)
            part[role, l] = part[role, l] + value if add else value

    def chunk(c):
        return pl.ds(c * per, per)

    def end_copy(role, c):
        return remote(
            part.at[role, chunk(c)],
            from_end.at[role, chunk(c)],
            out_sem.at[role, c],
            end_sem.at[role, c],
            (group, inner),
        )

    def other_copy(role, c):
        return remote(
            part.at[role, chunk(c)],
            from_other.at[role, chunk(c)],
            out_sem.at[role, c],
            other_sem.at[role, c],
            (group, other),
        )

    def back_copy(c):
        return remote(
            part.at[END, chunk(c)],
            from_other.at[1, chunk(c)],
            back_sem.at[c],
            other_sem.at[1, c],
            (group, end),
        )

    def relay(role, c):
        @pl.when(is_inner)
        def _():
            end_copy(role, c).wait_recv()
            part[role, chunk(c)] += from_end[role, chunk(c)]
            other_copy(role, c).start()

    def relay_back(c):
        @pl.when(is_inner)
        def _():
            other_copy(0, c).wait_recv()
            part[END, chunk(c)] += from_other[0, chunk(c)]
            back_copy(c).start()

    items = [(role, c) for role in (FAR, SECOND) for c in range(CHUNKS)]

    def pump(upto):
        @pl.when(is_end)
        def _():
            for i in range(pumped[0], upto):
                if i >= FLIGHT:
                    end_copy(*items[i - FLIGHT]).wait_send()
                end_copy(*items[i]).start()

        pumped[0] = upto

    pumped = [0]
    compute(n - 1 - end, laid, FAR)
    pump(FLIGHT)
    compute(other, laid, SECOND)
    pump(FLIGHT + 1)

    mids[me] = mid[...]
    for d in range(1, n):
        mid_copy(d).wait_recv()
    total = dot3(top_transfer[0], mids[0], TN)
    for s in range(1, n):
        total += dot3(top_transfer[s], mids[s], TN)
    mine = pl.ds(pl.multiple_of(me * share, share), share)
    top_own[mine, :] = total

    def top_copy(d):
        return remote(
            top_own.at[mine],
            top_own.at[mine],
            top_sem.at[0, d - 1],
            top_sem.at[1, d - 1],
            (group, lax.rem(me + d, n)),
        )

    for d in range(1, n):
        top_copy(d).start()

    pump(FLIGHT + 2)

    @pl.when(is_inner)
    def _():
        compute(end, laid, END)

    relay(FAR, 0)
    compute(me, laid, OWN)
    pump(FLIGHT + 3)
    relay(FAR, 1)

    def all_copy(d):
        return remote(
            top_own,
            tops.at[group],
            all_sem.at[0, d - 1],
            all_sem.at[1, d - 1],
            (lax.rem(group + d, groups), me),
        )

    for d in range(1, n):
        top_copy(d).wait_recv()
    for d in range(1, groups):
        all_copy(d).start()
    tops[group] = top_own[...]
    pump(FLIGHT + 4)
    relay(FAR, 2)
    relay_back(0)
    pump(FLIGHT + 5)
    relay(FAR, 3)
    relay_back(1)

    for d in range(1, groups):
        all_copy(d).wait_recv()
    field = jnp.zeros((share, mid.shape[1]), F32)
    for k in range(partner.shape[0]):
        p = tops[partner[k]]
        field += dot3(coupling[k, 0], p) + dot3(coupling[k, 1], rotated(p))
    for s in range(n):
        shares[s] = dot3(top_transfer[s], field)

    def down_copy(d):
        there = lax.rem(me + d, n)
        return remote(
            shares.at[there],
            shares_in.at[me],
            down_sem.at[0, d - 1],
            down_sem.at[1, d - 1],
            (group, there),
        )

    for d in range(1, n):
        down_copy(d).start()

    pump(FLIGHT + 6)
    relay(FAR, 4)
    relay_back(2)
    pump(FLIGHT + 7)
    relay(FAR, 5)
    relay_back(3)
    relay(FAR, 6)
    relay_back(4)
    pump(FLIGHT + 8)

    for side in range(2):
        @pl.when(takes_ext[side])
        def _(side=side):
            ext_copy(side).wait_recv()

            @pl.loop(0, leaves, unroll=2)
            def _(l):
                lay_out(laid_ext, (0 if side == 0 else 2 * leaves) + l, ext_in[side, l])

    @pl.when(is_inner)
    def _():
        @pl.loop(0, leaves, unroll=2)
        def _(l):
            lay_out(laid_ext, leaves + l, ext[l])

        compute(n, laid_ext, OWN, add=True)

    pump(FLIGHT + 9)
    relay(FAR, 7)
    relay_back(5)
    relay(SECOND, 0)
    relay_back(6)

    shares_in[me] = shares[me]
    for d in range(1, n):
        down_copy(d).wait_recv()
    total = shares_in[0]
    for s in range(1, n):
        total += shares_in[s]
    down[...] = total

    @pl.loop(0, leaves, unroll=2)
    def _(l):
        part[OWN, l] += dot3(transfer[l], down[...])

    def finish(c):
        other_copy(1, c).wait_recv()
        for i in range(per):
            l = c * per + i
            field = part[OWN, l] + from_other[1, l]
            out[l] = dot3(masked(basis[l], rank[l]), field) + near_part[l]

    pump(FLIGHT + 10)
    relay(SECOND, 1)
    relay_back(7)
    pump(FLIGHT + 11)
    for c in range(2, CHUNKS):
        pump(min(2 * CHUNKS, FLIGHT + 10 + c))
        relay(SECOND, c)
        finish(c - 2)
    finish(CHUNKS - 2)
    finish(CHUNKS - 1)

    for side in range(2):
        @pl.when(sends_ext[side])
        def _(side=side):
            ext_copy(side).wait_send()
    for d in range(1, n):
        mid_copy(d).wait_send()
        top_copy(d).wait_send()
        down_copy(d).wait_send()
    for d in range(1, groups):
        all_copy(d).wait_send()
    for c in range(CHUNKS):
        @pl.when(is_inner)
        def _(c=c):
            other_copy(FAR, c).wait_send()
            other_copy(SECOND, c).wait_send()
            back_copy(c).wait_send()

    @pl.when(is_end)
    def _():
        for item in items[-FLIGHT:]:
            end_copy(*item).wait_send()


def fields(slots, last, partner, rank, coefs, tables, own_parts, top_parts):
    own, prev, nxt, ext = coefs
    leaves, width, cols = own.shape
    count = slots.shape[2]
    n = lax.axis_size("sub")
    groups = lax.axis_size("leaf")
    unroll = max(u for u in range(1, 7) if count % u == 0)
    block = lambda *lead: pltpu.VMEM(lead + (width, cols), F32)
    dma = lambda *shape: pltpu.SemaphoreType.DMA(shape)
    operands = [*coefs, *tables, *own_parts, *top_parts]
    return pl.pallas_call(
        functools.partial(fields_kernel, unroll),
        in_specs=[SMEM] * 4 + [VMEM] * len(operands),
        out_specs=VMEM,
        out_shape=jax.ShapeDtypeStruct((leaves, width, cols), F32),
        scratch_shapes=[
            pltpu.VMEM((3 * leaves, 2 * width, 2 * cols), BF16),
            pltpu.VMEM((3 * leaves, 2 * width, 2 * cols), BF16),
            block(2, leaves),
            block(count),
            block(4, leaves),
            block(2, leaves),
            block(2, leaves),
            block(n),
            block(),
            block(groups),
            block(n),
            block(n),
            block(),
            dma(2, CHUNKS),
            dma(2, CHUNKS),
            dma(2, CHUNKS),
            dma(CHUNKS),
            dma(2, 2),
            dma(2, n - 1),
            dma(2, n - 1),
            dma(2, groups - 1),
            dma(2, n - 1),
        ],
        compiler_params=pltpu.CompilerParams(
            vmem_limit_bytes=60 * 1024 * 1024, collective_id=0, has_side_effects=True
        ),
        cost_estimate=cost(5 * count * 12 * width * width * cols, 12 * 2 ** 20),
        name="fields",
    )(slots, last, partner, rank, *operands)


def per_device(
    currents,
    leaf_basis,
    leaf_rank,
    leaf_transfer,
    top_transfer,
    far_table,
    send_src,
    recv_tgt,
    recv_type,
    top_coupling,
    top_list,
    near_blocks,
    near_tgt,
    near_src,
):
    leaves, panel, width = leaf_basis.shape
    cols = currents.shape[1]
    n = lax.axis_size("sub")
    me = lax.axis_index("sub")
    cur = currents.reshape(leaves, panel, cols)
    ends = [(0, 1), (n - 1, n - 2)]
    inner = jnp.where(me < n // 2, 1, n - 2)
    end = jnp.where(me < n // 2, 0, n - 1)

    below_rim = shifted(cur[leaves - HALO_L :], ("leaf", "sub"), 1)
    above_rim = shifted(cur[:HALO_L], ("leaf", "sub"), -1)
    recv = jnp.stack([recv_tgt[0], recv_type[0]])
    theirs = lax.all_to_all(jnp.moveaxis(recv, 2, 0), "sub", 0, 0)
    sources = send_src[0]
    sources = jnp.stack(
        [shifted(sources[2], "leaf", 1), sources[1] + leaves, shifted(sources[0], "leaf", -1) + 2 * leaves]
    )
    extra_src = lax.ppermute(lax.dynamic_index_in_dim(sources, inner, 1, False), "sub", ends)
    extra = lax.dynamic_index_in_dim(recv, end, 2, False)
    flat = lambda x: x.reshape(x.shape[0], -1)
    both = jnp.concatenate([theirs, extra[None]], axis=0)
    all_src = jnp.concatenate([jnp.moveaxis(sources, 1, 0), extra_src[None]], axis=0)
    slots, last = ordered(flat(both[:, 0]), flat(all_src), flat(both[:, 1]), leaves)

    coef, mid = up(leaf_rank, cur, leaf_basis, leaf_transfer)
    prev, nxt = shifted(coef, "leaf", 1), shifted(coef, "leaf", -1)
    ext = lax.ppermute(coef, "sub", ends)
    tables = split_table(far_table)
    near_part = near(near_tgt[0], near_src[0], below_rim, cur, above_rim, near_blocks)
    out = fields(
        slots,
        last,
        top_list[0],
        leaf_rank,
        [coef, prev, nxt, ext],
        tables,
        [leaf_basis, leaf_transfer, near_part],
        [mid, top_transfer[0], top_coupling[0]],
    )
    return out.reshape(leaves * panel, cols)


def solution(mesh):
    placed = (
        P(("leaf", "sub"), None),
        P(("leaf", "sub"), None, None),
        P(("leaf", "sub")),
        P(("leaf", "sub"), None, None),
        P("leaf", None, None, "sub"),
        P(),
        P(("leaf", "sub"), None, None, None),
        P(("leaf", "sub"), None, None, None),
        P(("leaf", "sub"), None, None, None),
        P("leaf", None, None, "sub", None),
        P("leaf", None),
        P(("leaf", "sub"), None, None, None),
        P(("leaf", "sub"), None),
        P(("leaf", "sub"), None),
    )
    return jax.shard_map(
        per_device, mesh=mesh, in_specs=placed, out_specs=P(("leaf", "sub"), None), check_vma=False
    )
```

```python
import functools

import jax
import jax.numpy as jnp
from jax import lax
from jax.experimental import pallas as pl
from jax.experimental.pallas import tpu as pltpu
from jax.sharding import PartitionSpec as P

HALO_L = 4
F32 = jnp.float32
BF16 = jnp.bfloat16
NN = (((1,), (0,)), ((), ()))
TN = (((0,), (0,)), ((), ()))

SMEM = pl.BlockSpec(memory_space=pltpu.SMEM)
VMEM = pl.BlockSpec(memory_space=pltpu.VMEM)
ANY = pl.BlockSpec(memory_space=pl.ANY)
MESH = pl.DeviceIdType.MESH


def split(x):
    high = x.astype(BF16)
    return high, (x - high.astype(F32)).astype(BF16)


def dot(a, b, dims=NN):
    return lax.dot_general(a, b, dims, preferred_element_type=F32)


def dot3(a, b, dims=NN):
    ah, al = split(a)
    bh, bl = split(b)
    return dot(ah, bh, dims) + (dot(ah, bl, dims) + dot(al, bh, dims))


def rotated(c):
    half = c.shape[-1] // 2
    lane = lax.broadcasted_iota(jnp.int32, c.shape, c.ndim - 1)
    turned_c = pltpu.roll(c, half, c.ndim - 1)
    return jnp.where(lane < half, -turned_c, turned_c)


def lay_out(store, at, c):
    rows, cols = c.shape
    high, low = split(c)
    rhigh, rlow = split(rotated(c))
    store[at, :rows, :cols] = high
    store[at, :rows, cols:] = low
    store[at, rows:, :cols] = rhigh
    store[at, rows:, cols:] = rlow


def applied(mh, ml, b):
    cols = b.shape[1] // 2
    p = dot(mh, b)
    return p[:, :cols] + (p[:, cols:] + dot(ml, b[:, :cols]))


def masked(basis, rank):
    lane = lax.broadcasted_iota(jnp.int32, basis.shape, 1)
    return jnp.where(lane < rank, basis, 0.0)


CHUNKS = 8
FLIGHT = 2
PARTS = 4
FAR, SECOND, END, OWN = range(4)
NEXT, PREV, SIDE = range(3)


def ordered(tgt, src, kind, count, leaves, spare):
    rows = -(-count // 8) * 8
    lane = lax.broadcasted_iota(jnp.int32, (rows, 128), 1)
    line = lax.broadcasted_iota(jnp.int32, (rows, 128), 0)
    spot = lax.broadcasted_iota(jnp.int32, (1, 128), 1)
    src = jnp.where(tgt < 0, spare, src).astype(F32)
    key = jnp.where(tgt < 0, leaves, tgt)
    key = jnp.where(spot < count, key, leaves + 1).astype(F32)
    stood = lambda x: jnp.sum(jnp.where(line == lane, x, 0.0), axis=1, keepdims=True)
    key_at = stood(key)
    before = (key < key_at) | ((key == key_at) & (lane < line))
    place = jnp.sum(jnp.where(before, 1.0, 0.0), axis=1, keepdims=True)
    hot = (place == lane.astype(F32)) & (line < count)
    pick = lambda x: jnp.sum(jnp.where(hot, stood(x), 0.0), axis=0, keepdims=True)
    key, src, kind = pick(key), pick(src), pick(kind.astype(F32))
    wide = jnp.broadcast_to(key, (8, 128))
    keep = jnp.where((wide == pltpu.roll(wide, 1, 1))[:1] & (spot > 0), 1.0, 0.0)
    wide = (leaves, 128)
    lane = lax.broadcasted_iota(jnp.int32, wide, 1)
    line = lax.broadcasted_iota(jnp.int32, wide, 0)
    found = (key == line.astype(F32)) & (lane < count)
    last = jnp.max(jnp.where(found, lane.astype(F32), -1.0), axis=1, keepdims=True)
    last = jnp.sum(jnp.where(line == lane, last, 0.0), axis=0, keepdims=True)
    return [x.astype(jnp.int32) for x in (src, kind, keep, last)]


def within(i, ref):
    return jnp.clip(i, 0, ref.shape[0] - 1)


def field_kernel(
    slots_count,
    partner,
    rank,
    send_src,
    recv_tgt,
    recv_type,
    near_tgt,
    near_src,
    shares,
    coupling,
    cur_in,
    basis_in,
    transfer_in,
    blocks_in,
    table_in,
    out,
    cur,
    basis,
    transfer,
    blocks,
    table,
    high,
    low,
    coef,
    raw,
    ext_in,
    rim,
    laid,
    laid_ext,
    runs,
    part,
    from_end,
    from_other,
    near_part,
    whole,
    mid,
    top_part,
    top_in,
    top_own,
    tops,
    field_own,
    numbers,
    sources,
    sub_in,
    src_in,
    src_sum,
    ext_src,
    near_rows,
    far_rows,
    near_slots,
    slots,
    load_sem,
    block_sem,
    table_sem,
    rows_sem,
    rim_sem,
    number_sem,
    source_sem,
    ext_src_sem,
    raw_sem,
    ext_sem,
    whole_sem,
    share_sem,
    top_sem,
    all_sem,
    field_sem,
    out_sem,
    end_sem,
    other_sem,
    back_sem,
):
    n = lax.axis_size("sub")
    groups = lax.axis_size("leaf")
    me = lax.axis_index("sub")
    group = lax.axis_index("leaf")
    leaves = cur.shape[0]
    halo = rim.shape[1]
    count = slots_count
    near_count = blocks.shape[0]
    per = leaves // CHUNKS
    up_per = leaves // PARTS
    share = whole.shape[0] // n
    low_side = me < n // 2
    is_end = (me == 0) | (me == n - 1)
    is_inner = (me != 0) & (me != n - 1)
    end = jnp.where(low_side, 0, n - 1)
    inner = jnp.where(low_side, 1, n - 2)
    other = n - 1 - inner
    has_up = group + 1 < groups
    has_down = group > 0
    has_after = has_up | (me < n - 1)
    has_before = has_down | (me > 0)
    up_group = jnp.minimum(group + 1, groups - 1)
    down_group = jnp.maximum(group - 1, 0)
    after = (jnp.where(me < n - 1, group, up_group), lax.rem(me + 1, n))
    before = (jnp.where(me > 0, group, down_group), lax.rem(me + n - 1, n))

    barrier = pltpu.get_barrier_semaphore()

    def greet(device):
        pl.semaphore_signal(barrier, inc=1, device_id=device, device_id_type=MESH)

    for d in range(1, n):
        greet((group, lax.rem(me + d, n)))
    for d in range(1, groups):
        greet((lax.rem(group + d, groups), me))
    cross_after = (me == n - 1) & has_up
    cross_before = (me == 0) & has_down

    @pl.when(cross_after)
    def _():
        greet(after)

    @pl.when(cross_before)
    def _():
        greet(before)

    def up_chunk(p):
        return pl.ds(p * up_per, up_per)

    def load(i, p):
        source, target = ((cur_in, cur), (basis_in, basis), (transfer_in, transfer))[i]
        return pltpu.make_async_copy(
            source.at[up_chunk(p)], target.at[up_chunk(p)], load_sem.at[i, p]
        )

    for p in range(PARTS):
        for i in range(3):
            load(i, p).start()

    def block_load(p):
        span = pl.ds(p * (near_count // PARTS), near_count // PARTS)
        return pltpu.make_async_copy(blocks_in.at[span], blocks.at[span], block_sem.at[p])

    def table_load(p):
        span = pl.ds(p * (table.shape[0] // PARTS), table.shape[0] // PARTS)
        return pltpu.make_async_copy(table_in.at[span], table.at[span], table_sem.at[p])

    for p in range(PARTS):
        block_load(p).start()
    for p in range(PARTS):
        table_load(p).start()

    cap = send_src.shape[2]
    padded = lambda *parts: jnp.concatenate(
        [*parts, jnp.zeros((parts[0].shape[0], 128 - sum(x.shape[1] for x in parts)), jnp.int32)],
        axis=1,
    )
    triple = lambda ref: padded(*(ref[o] for o in range(3)))
    numbers[:n, :] = triple(recv_tgt)
    numbers[n:, :] = triple(recv_type)
    sources[:n, :] = triple(send_src)
    sources[n:, :] = jnp.zeros((8 - n, 128), jnp.int32)
    near_kind = lax.broadcasted_iota(jnp.int32, (1, 128), 1)
    for i, row in enumerate(
        ordered(padded(near_tgt[...]), padded(near_src[...]), near_kind, near_count, leaves, 0)
    ):
        near_rows[i : i + 1, :] = row
    near_copy = pltpu.make_async_copy(near_rows, near_slots, rows_sem.at[0])

    pl.semaphore_wait(
        barrier, n + groups - 2 + jnp.where(cross_after, 1, 0) + jnp.where(cross_before, 1, 0)
    )
    near_copy.start()

    def remote(source, target, sems, at, device):
        return pltpu.make_async_remote_copy(
            src_ref=source,
            dst_ref=target,
            send_sem=sems.at[(0, *at)],
            recv_sem=sems.at[(1, *at)],
            device_id=device,
            device_id_type=MESH,
        )

    def sub_peer(d):
        return (group, lax.rem(me + d, n))

    def rim_copy(side):
        if side == 0:
            return remote(cur_in.at[pl.ds(leaves - halo, halo)], rim.at[0], rim_sem, (0,), after)
        return remote(cur_in.at[pl.ds(0, halo)], rim.at[1], rim_sem, (1,), before)

    sends_rim = [has_after, has_before]
    takes_rim = [has_before, has_after]
    for side in range(2):
        @pl.when(sends_rim[side])
        def _(side=side):
            rim_copy(side).start()

        @pl.when(jnp.logical_not(takes_rim[side]))
        def _(side=side):
            rim[side] = jnp.zeros(rim.shape[1:], F32)

    def number_copy(d):
        return remote(
            numbers, sub_in.at[me], number_sem, (d - 1,), sub_peer(d)
        )

    def whole_copy(d):
        mine = pl.ds(pl.multiple_of(me * share, share), share)
        return remote(
            shares.at[lax.rem(me + d, n)], whole.at[mine], whole_sem, (d - 1,), sub_peer(d)
        )

    for d in range(1, n):
        number_copy(d).start()
        whole_copy(d).start()

    def source_copy(side):
        there = (up_group, me) if side == 0 else (down_group, me)
        return remote(sources, src_in.at[side], source_sem, (side,), there)

    sends_leaf = [has_up, has_down]
    takes_leaf = [has_down, has_up]
    for side in range(2):
        @pl.when(sends_leaf[side])
        def _(side=side):
            source_copy(side).start()

        @pl.when(jnp.logical_not(takes_leaf[side]))
        def _(side=side):
            src_in[side] = jnp.zeros(src_in.shape[1:], jnp.int32)
            raw[side] = jnp.zeros(raw.shape[1:], F32)

    def raw_copy(to, p):
        there = {NEXT: (up_group, me), PREV: (down_group, me), SIDE: (group, inner)}[to]
        return remote(coef.at[up_chunk(p)], raw.at[to, up_chunk(p)], raw_sem, (to, p), there)

    sends_raw = [has_up, has_down, is_end]
    takes_raw = [has_down, has_up, is_inner]

    def send_raw(p):
        for to in range(3):
            @pl.when(sends_raw[to])
            def _(to=to):
                raw_copy(to, p).start()

    total = jnp.zeros(mid.shape, F32)
    for p in range(PARTS):
        for i in range(3):
            load(i, p).wait()
        for i in range(up_per):
            l = p * up_per + i
            c = dot3(masked(basis[l], rank[l]), cur[l], TN)
            coef[l] = c
            total += dot3(transfer[l], c, TN)
        if p:
            send_raw(p - 1)
    mid[...] = total
    mine = pl.ds(pl.multiple_of(me * share, share), share)
    whole[mine, :] = shares[me]
    for d in range(1, n):
        whole_copy(d).wait_recv()
    send_raw(PARTS - 1)
    top_part[...] = dot3(whole[...], mid[...])

    for side in range(2):
        @pl.when(takes_rim[side])
        def _(side=side):
            rim_copy(side).wait_recv()

    def share_copy(d):
        there = lax.rem(me + d, n)
        span = pl.ds(pl.multiple_of(there * share, share), share)
        return remote(top_part.at[span], top_in.at[me], share_sem, (d - 1,), sub_peer(d))

    @pl.loop(0, halo)
    def _(l):
        lay_out(laid_ext, l, rim[0, l])
        lay_out(laid_ext, halo + leaves + l, rim[1, l])

    @pl.loop(0, leaves, unroll=2)
    def _(l):
        lay_out(laid_ext, halo + l, cur[l])

    for d in range(1, n):
        share_copy(d).start()

    def gather(rows, at, store):
        @pl.loop(0, leaves, unroll=2)
        def _(l):
            j = rows[4 * at + 3, l]
            store(l, runs[within(j, runs)] * jnp.where(j >= 0, 1.0, 0.0))

    def in_order(rows, at, number, product):
        unroll = max(u for u in range(1, 7) if number % u == 0)

        def step(i, acc):
            spots = [i * unroll + u for u in range(unroll)]
            results = [product(rows[4 * at, j], rows[4 * at + 1, j]) for j in spots]
            for j, result in zip(spots, results):
                acc = acc * rows[4 * at + 2, j].astype(F32) + result
                runs[j] = acc
            return acc

        lax.fori_loop(0, number // unroll, step, jnp.zeros(runs.shape[1:], F32))

    def near_product(s, k):
        k = within(k, blocks)
        h0, l0 = split(blocks[k, 0])
        h1, l1 = split(blocks[k, 1])
        b = laid_ext[within(s, laid_ext)]
        return applied(jnp.concatenate([h0, h1], axis=1), jnp.concatenate([l0, l1], axis=1), b)

    def put_near(l, value):
        near_part[l] = value

    near_copy.wait()
    for p in range(PARTS):
        block_load(p).wait()
    in_order(near_slots, 0, near_count, near_product)
    gather(near_slots, 0, put_near)

    top_in[me] = top_part[mine, :]
    for d in range(1, n):
        share_copy(d).wait_recv()
    total = top_in[0]
    for s in range(1, n):
        total += top_in[s]
    top_own[mine, :] = total

    for side in range(2):
        @pl.when(takes_leaf[side])
        def _(side=side):
            source_copy(side).wait_recv()

    spot = lax.broadcasted_iota(jnp.int32, (8, 128), 1)
    src_sum[...] = jnp.where(
        spot < cap,
        pltpu.roll(src_in[0], 128 - 2 * cap, 1),
        jnp.where(
            spot < 2 * cap, sources[...] + leaves, pltpu.roll(src_in[1], 2 * cap, 1) + 2 * leaves
        ),
    )

    for p in range(PARTS):
        table_load(p).wait()

    @pl.loop(0, table.shape[0])
    def _(i):
        w = table.shape[3]
        h0, l0 = split(table[i, 0])
        h1, l1 = split(table[i, 1])
        high[i, :, :w] = h0
        high[i, :, w:] = h1
        low[i, :, :w] = l0
        low[i, :, w:] = l1

    def top_copy(d):
        return remote(top_own.at[mine], top_own.at[mine], top_sem, (d - 1,), sub_peer(d))

    for d in range(1, n):
        top_copy(d).start()

    ext_src_copy = remote(src_sum, ext_src, ext_src_sem, (), (group, inner))

    @pl.when(is_end)
    def _():
        ext_src_copy.start()
        ext_src[...] = jnp.zeros(ext_src.shape, jnp.int32)

    @pl.loop(0, leaves, unroll=2)
    def _(l):
        lay_out(laid, leaves + l, coef[l])

    sub_in[me] = numbers[...]
    for d in range(1, n):
        number_copy(d).wait_recv()

    @pl.when(is_inner)
    def _():
        ext_src_copy.wait_recv()

    for s in range(n + 1):
        if s < n:
            args = sub_in[s, pl.ds(me, 1)], src_sum[s : s + 1], sub_in[s, pl.ds(n + me, 1)]
        else:
            args = numbers[pl.ds(end, 1)], ext_src[pl.ds(me, 1)], numbers[pl.ds(n + end, 1)]
        for i, row in enumerate(ordered(*args, count, leaves, leaves)):
            far_rows[4 * s + i : 4 * s + i + 1, :] = row
    far_copy = pltpu.make_async_copy(far_rows, slots, rows_sem.at[1])

    for to in (NEXT, PREV):
        @pl.when(takes_raw[to])
        def _(to=to):
            for p in range(PARTS):
                raw_copy(to, p).wait_recv()

    far_copy.start()

    @pl.loop(0, leaves, unroll=2)
    def _(l):
        lay_out(laid, l, raw[NEXT, l])
        lay_out(laid, 2 * leaves + l, raw[PREV, l])

    far_copy.wait()

    def compute(at, store, role, add=False):
        def product(s, k):
            k = within(k, high)
            return applied(high[k], low[k], store[within(s, store)])

        in_order(slots, at, count, product)

        def put(l, value):
            part[role, l] = part[role, l] + value if add else value

        gather(slots, at, put)

    def chunk(c):
        return pl.ds(c * per, per)

    def end_copy(role, c):
        return pltpu.make_async_remote_copy(
            src_ref=part.at[role, chunk(c)],
            dst_ref=from_end.at[role, chunk(c)],
            send_sem=out_sem.at[role, c],
            recv_sem=end_sem.at[role, c],
            device_id=(group, inner),
            device_id_type=MESH,
        )

    def other_copy(role, c):
        return pltpu.make_async_remote_copy(
            src_ref=part.at[role, chunk(c)],
            dst_ref=from_other.at[role, chunk(c)],
            send_sem=out_sem.at[role, c],
            recv_sem=other_sem.at[role, c],
            device_id=(group, other),
            device_id_type=MESH,
        )

    def back_copy(c):
        return pltpu.make_async_remote_copy(
            src_ref=part.at[END, chunk(c)],
            dst_ref=from_other.at[1, chunk(c)],
            send_sem=back_sem.at[c],
            recv_sem=other_sem.at[1, c],
            device_id=(group, end),
            device_id_type=MESH,
        )

    def relay(role, c):
        @pl.when(is_inner)
        def _():
            end_copy(role, c).wait_recv()
            part[role, chunk(c)] += from_end[role, chunk(c)]
            other_copy(role, c).start()

    def relay_back(c):
        @pl.when(is_inner)
        def _():
            other_copy(0, c).wait_recv()
            part[END, chunk(c)] += from_other[0, chunk(c)]
            back_copy(c).start()

    items = [(role, c) for role in (FAR, SECOND) for c in range(CHUNKS)]
    pumped = [0]

    def pump(upto):
        upto = min(upto, len(items))

        @pl.when(is_end)
        def _():
            for i in range(pumped[0], upto):
                if i >= FLIGHT:
                    end_copy(*items[i - FLIGHT]).wait_send()
                end_copy(*items[i]).start()

        pumped[0] = upto

    compute(n - 1 - end, laid, FAR)
    pump(FLIGHT)
    compute(other, laid, SECOND)
    pump(FLIGHT + 1)

    def ext_copy(side):
        there = (up_group, me) if side == 0 else (down_group, me)
        return remote(raw.at[SIDE], ext_in.at[side], ext_sem, (side,), there)

    sends_ext = [is_inner & has_up, is_inner & has_down]
    takes_ext = [is_inner & has_down, is_inner & has_up]

    def all_copy(d):
        return remote(
            top_own, tops.at[group], all_sem, (d - 1,), (lax.rem(group + d, groups), me)
        )

    for d in range(1, n):
        top_copy(d).wait_recv()
    for d in range(1, groups):
        all_copy(d).start()
    tops[group] = top_own[...]

    @pl.when(is_inner)
    def _():
        for p in range(PARTS):
            raw_copy(SIDE, p).wait_recv()

    for side in range(2):
        @pl.when(sends_ext[side])
        def _(side=side):
            ext_copy(side).start()

    @pl.when(is_inner)
    def _():
        compute(end, laid, END)

    pump(FLIGHT + 2)
    relay(FAR, 0)
    compute(me, laid, OWN)
    pump(FLIGHT + 3)
    relay(FAR, 1)
    pump(FLIGHT + 4)
    relay(FAR, 2)
    relay_back(0)
    pump(FLIGHT + 5)
    relay(FAR, 3)
    relay_back(1)
    pump(FLIGHT + 6)

    for d in range(1, groups):
        all_copy(d).wait_recv()
    field = jnp.zeros((share, mid.shape[1]), F32)
    for k in range(partner.shape[0]):
        p = tops[within(partner[k], tops)]
        field += dot3(coupling[k, 0], p) + dot3(coupling[k, 1], rotated(p))
    field_own[mine, :] = field

    def field_copy(d):
        return remote(field_own.at[mine], field_own.at[mine], field_sem, (d - 1,), sub_peer(d))

    relay(FAR, 4)
    relay_back(2)
    for d in range(1, n):
        field_copy(d).start()
    pump(FLIGHT + 7)
    relay(FAR, 5)
    relay_back(3)
    pump(FLIGHT + 8)
    relay(FAR, 6)
    relay_back(4)
    pump(FLIGHT + 9)
    relay(FAR, 7)
    relay_back(5)
    pump(FLIGHT + 10)

    for d in range(1, n):
        field_copy(d).wait_recv()
    mid[...] = dot3(whole[...], field_own[...], TN)

    @pl.loop(0, leaves, unroll=2)
    def _(l):
        part[OWN, l] += dot3(transfer[l], mid[...])

    relay(SECOND, 0)
    relay_back(6)
    pump(FLIGHT + 11)

    def lay_ext(to, at, ref):
        @pl.loop(0, leaves, unroll=2)
        def _(l):
            lay_out(laid_ext, at * leaves + l, ref[to, l])

    @pl.when(is_inner)
    def _():
        lay_ext(SIDE, 1, raw)

    relay(SECOND, 1)
    relay_back(7)
    pump(FLIGHT + 12)
    for side in range(2):
        @pl.when(takes_ext[side])
        def _(side=side):
            ext_copy(side).wait_recv()
            lay_ext(side, 2 * side, ext_in)

    relay(SECOND, 2)
    pump(FLIGHT + 13)

    @pl.when(is_inner)
    def _():
        compute(n, laid_ext, OWN, add=True)

    def finish(c):
        other_copy(1, c).wait_recv()
        for i in range(per):
            l = c * per + i
            field = part[OWN, l] + from_other[1, l]
            out[l] = dot3(masked(basis[l], rank[l]), field) + near_part[l]

    relay(SECOND, 3)
    pump(FLIGHT + 14)
    done = 0
    for c in range(4, CHUNKS + 2):
        if c < CHUNKS:
            relay(SECOND, c)
        while done <= c - 2:
            finish(done)
            done += 1

    for side in range(2):
        @pl.when(sends_rim[side])
        def _(side=side):
            rim_copy(side).wait_send()

        @pl.when(sends_leaf[side])
        def _(side=side):
            source_copy(side).wait_send()

        @pl.when(sends_ext[side])
        def _(side=side):
            ext_copy(side).wait_send()

    for to in range(3):
        @pl.when(sends_raw[to])
        def _(to=to):
            for p in range(PARTS):
                raw_copy(to, p).wait_send()

    for d in range(1, n):
        number_copy(d).wait_send()
        whole_copy(d).wait_send()
        share_copy(d).wait_send()
        top_copy(d).wait_send()
        field_copy(d).wait_send()
    for d in range(1, groups):
        all_copy(d).wait_send()

    @pl.when(is_inner)
    def _():
        for c in range(CHUNKS):
            other_copy(FAR, c).wait_send()
            other_copy(SECOND, c).wait_send()
            back_copy(c).wait_send()

    @pl.when(is_end)
    def _():
        ext_src_copy.wait_send()
        for item in items[-FLIGHT:]:
            end_copy(*item).wait_send()


def fields(count, partner, rank, numbers, shares, coupling, cur, basis, transfer, blocks, table):
    leaves, width, cols = cur.shape
    kinds = table.shape[0]
    n = lax.axis_size("sub")
    groups = lax.axis_size("leaf")
    share = width // n
    f32 = lambda *shape: pltpu.VMEM(shape, F32)
    i32 = lambda *shape: pltpu.VMEM(shape, jnp.int32)
    b16 = lambda *shape: pltpu.VMEM(shape, BF16)
    block = lambda *lead: f32(*lead, width, cols)
    dma = lambda *shape: pltpu.SemaphoreType.DMA(shape)
    lists = 4 * (n + 1)
    lists = -(-lists // 8) * 8
    return pl.pallas_call(
        functools.partial(field_kernel, count),
        in_specs=[SMEM] * 2 + [VMEM] * 7 + [ANY] * 5,
        out_specs=VMEM,
        out_shape=jax.ShapeDtypeStruct((leaves, width, cols), F32),
        scratch_shapes=[
            block(leaves),
            f32(*basis.shape),
            f32(*transfer.shape),
            f32(*blocks.shape),
            f32(*table.shape),
            b16(kinds, width, 2 * width),
            b16(kinds, width, 2 * width),
            block(leaves),
            block(3, leaves),
            block(2, leaves),
            block(2, HALO_L),
            b16(3 * leaves, 2 * width, 2 * cols),
            b16(3 * leaves, 2 * width, 2 * cols),
            block(max(count, blocks.shape[0])),
            block(4, leaves),
            block(2, leaves),
            block(2, leaves),
            block(leaves),
            f32(width, width),
            block(),
            block(),
            f32(n, share, cols),
            block(),
            block(groups),
            block(),
            i32(2 * n, 128),
            i32(8, 128),
            i32(n, 2 * n, 128),
            i32(2, 8, 128),
            i32(8, 128),
            i32(8, 128),
            i32(8, 128),
            i32(lists, 128),
            pltpu.SMEM((8, 128), jnp.int32),
            pltpu.SMEM((lists, 128), jnp.int32),
            dma(3, PARTS),
            dma(PARTS),
            dma(PARTS),
            dma(2),
            dma(2, 2),
            dma(2, n - 1),
            dma(2, 2),
            dma(2),
            dma(2, 3, PARTS),
            dma(2, 2),
            dma(2, n - 1),
            dma(2, n - 1),
            dma(2, n - 1),
            dma(2, groups - 1),
            dma(2, n - 1),
            dma(2, CHUNKS),
            dma(2, CHUNKS),
            dma(2, CHUNKS),
            dma(CHUNKS),
        ],
        compiler_params=pltpu.CompilerParams(
            vmem_limit_bytes=67043328, collective_id=0, has_side_effects=True
        ),
        cost_estimate=pl.CostEstimate(
            flops=int(9 * count * 12 * width * width * cols),
            bytes_accessed=20 * 2 ** 20,
            transcendentals=0,
        ),
        name="fields",
    )(partner, rank, *numbers, shares, coupling, cur, basis, transfer, blocks, table)


def per_device(
    currents,
    leaf_basis,
    leaf_rank,
    leaf_transfer,
    top_transfer,
    far_table,
    send_src,
    recv_tgt,
    recv_type,
    top_coupling,
    top_list,
    near_blocks,
    near_tgt,
    near_src,
):
    leaves, panel, _ = leaf_basis.shape
    cols = currents.shape[1]
    out = fields(
        3 * send_src.shape[3],
        top_list[0],
        leaf_rank,
        [send_src[0], recv_tgt[0], recv_type[0], near_tgt, near_src],
        jnp.swapaxes(top_transfer[0], 1, 2),
        top_coupling[0],
        currents.reshape(leaves, panel, cols),
        leaf_basis,
        leaf_transfer,
        near_blocks,
        far_table,
    )
    return out.reshape(leaves * panel, cols)


def solution(mesh):
    placed = (
        P(("leaf", "sub"), None),
        P(("leaf", "sub"), None, None),
        P(("leaf", "sub")),
        P(("leaf", "sub"), None, None),
        P("leaf", None, None, "sub"),
        P(),
        P(("leaf", "sub"), None, None, None),
        P(("leaf", "sub"), None, None, None),
        P(("leaf", "sub"), None, None, None),
        P("leaf", None, None, "sub", None),
        P("leaf", None),
        P(("leaf", "sub"), None, None, None),
        P(("leaf", "sub"), None),
        P(("leaf", "sub"), None),
    )
    return jax.shard_map(
        per_device, mesh=mesh, in_specs=placed, out_specs=P(("leaf", "sub"), None), check_vma=False
    )
```

```python
import functools

import jax
import jax.numpy as jnp
from jax import lax
from jax.experimental import pallas as pl
from jax.experimental.pallas import tpu as pltpu
from jax.sharding import PartitionSpec as P

HALO_L = 4
F32 = jnp.float32
BF16 = jnp.bfloat16
NN = (((1,), (0,)), ((), ()))
TN = (((0,), (0,)), ((), ()))

SMEM = pl.BlockSpec(memory_space=pltpu.SMEM)
VMEM = pl.BlockSpec(memory_space=pltpu.VMEM)
ANY = pl.BlockSpec(memory_space=pl.ANY)
MESH = pl.DeviceIdType.MESH


def split(x):
    high = x.astype(BF16)
    return high, (x - high.astype(F32)).astype(BF16)


def dot(a, b, dims=NN):
    return lax.dot_general(a, b, dims, preferred_element_type=F32)


def dot3(a, b, dims=NN):
    ah, al = split(a)
    bh, bl = split(b)
    return dot(ah, bh, dims) + (dot(ah, bl, dims) + dot(al, bh, dims))


def rotated(c):
    half = c.shape[-1] // 2
    lane = lax.broadcasted_iota(jnp.int32, c.shape, c.ndim - 1)
    turned_c = pltpu.roll(c, half, c.ndim - 1)
    return jnp.where(lane < half, -turned_c, turned_c)


def lay_out(store, at, c):
    rows, cols = c.shape
    high, low = split(c)
    rhigh, rlow = split(rotated(c))
    store[at, :rows, :cols] = high
    store[at, :rows, cols:] = low
    store[at, rows:, :cols] = rhigh
    store[at, rows:, cols:] = rlow


def applied(mh, ml, b):
    cols = b.shape[1] // 2
    p = dot(mh, b)
    return p[:, :cols] + (p[:, cols:] + dot(ml, b[:, :cols]))


def masked(basis, rank):
    lane = lax.broadcasted_iota(jnp.int32, basis.shape, 1)
    return jnp.where(lane < rank, basis, 0.0)


CHUNKS = 8
FLIGHT = 2
AHEAD = 2
PARTS = 4
FAR, SECOND, END, OWN = range(4)
NEXT, PREV, SIDE = range(3)


def ordered(tgt, src, kind, count, leaves, spare):
    rows = -(-count // 8) * 8
    lane = lax.broadcasted_iota(jnp.int32, (rows, 128), 1)
    line = lax.broadcasted_iota(jnp.int32, (rows, 128), 0)
    spot = lax.broadcasted_iota(jnp.int32, (1, 128), 1)
    src = jnp.where(tgt < 0, spare, src).astype(F32)
    key = jnp.where(tgt < 0, leaves, tgt)
    key = jnp.where(spot < count, key, leaves + 1).astype(F32)
    stood = lambda x: jnp.sum(jnp.where(line == lane, x, 0.0), axis=1, keepdims=True)
    key_at = stood(key)
    before = (key < key_at) | ((key == key_at) & (lane < line))
    place = jnp.sum(jnp.where(before, 1.0, 0.0), axis=1, keepdims=True)
    hot = (place == lane.astype(F32)) & (line < count)
    pick = lambda x: jnp.sum(jnp.where(hot, stood(x), 0.0), axis=0, keepdims=True)
    key, src, kind = pick(key), pick(src), pick(kind.astype(F32))
    wide = jnp.broadcast_to(key, (8, 128))
    keep = jnp.where((wide == pltpu.roll(wide, 1, 1))[:1] & (spot > 0), 1.0, 0.0)
    wide = (leaves, 128)
    lane = lax.broadcasted_iota(jnp.int32, wide, 1)
    line = lax.broadcasted_iota(jnp.int32, wide, 0)
    found = (key == line.astype(F32)) & (lane < count)
    last = jnp.max(jnp.where(found, lane.astype(F32), -1.0), axis=1, keepdims=True)
    last = jnp.sum(jnp.where(line == lane, last, 0.0), axis=0, keepdims=True)
    return [x.astype(jnp.int32) for x in (src, kind, keep, last)]


def within(i, ref):
    return jnp.clip(i, 0, ref.shape[0] - 1)


def field_kernel(
    slots_count,
    partner,
    rank,
    send_src,
    recv_tgt,
    recv_type,
    near_tgt,
    near_src,
    shares,
    coupling,
    cur_in,
    basis_in,
    transfer_in,
    blocks_in,
    table_in,
    out,
    cur,
    basis,
    transfer,
    blocks,
    table,
    high,
    low,
    coef,
    raw,
    ext_in,
    rim,
    laid,
    laid_ext,
    laid_near,
    runs,
    part,
    from_end,
    from_other,
    near_part,
    whole,
    mid,
    top_part,
    top_in,
    top_own,
    tops,
    field_own,
    numbers,
    sources,
    sub_in,
    src_in,
    src_sum,
    ext_src,
    near_rows,
    far_rows,
    ext_rows,
    near_slots,
    slots,
    ext_slots,
    load_sem,
    block_sem,
    table_sem,
    rows_sem,
    rim_sem,
    number_sem,
    source_sem,
    ext_src_sem,
    raw_sem,
    ext_sem,
    whole_sem,
    share_sem,
    top_sem,
    all_sem,
    field_sem,
    out_sem,
    end_sem,
    other_sem,
    back_sem,
):
    n = lax.axis_size("sub")
    groups = lax.axis_size("leaf")
    me = lax.axis_index("sub")
    group = lax.axis_index("leaf")
    leaves = cur.shape[0]
    halo = rim.shape[1]
    count = slots_count
    near_count = blocks.shape[0]
    per = leaves // CHUNKS
    up_per = leaves // PARTS
    share = whole.shape[0] // n
    low_side = me < n // 2
    is_end = (me == 0) | (me == n - 1)
    is_inner = (me != 0) & (me != n - 1)
    end = jnp.where(low_side, 0, n - 1)
    inner = jnp.where(low_side, 1, n - 2)
    other = n - 1 - inner
    has_up = group + 1 < groups
    has_down = group > 0
    has_after = has_up | (me < n - 1)
    has_before = has_down | (me > 0)
    up_group = jnp.minimum(group + 1, groups - 1)
    down_group = jnp.maximum(group - 1, 0)
    after = (jnp.where(me < n - 1, group, up_group), lax.rem(me + 1, n))
    before = (jnp.where(me > 0, group, down_group), lax.rem(me + n - 1, n))

    barrier = pltpu.get_barrier_semaphore()

    def greet(device):
        pl.semaphore_signal(barrier, inc=1, device_id=device, device_id_type=MESH)

    for d in range(1, n):
        greet((group, lax.rem(me + d, n)))
    for d in range(1, groups):
        greet((lax.rem(group + d, groups), me))
    cross_after = (me == n - 1) & has_up
    cross_before = (me == 0) & has_down

    @pl.when(cross_after)
    def _():
        greet(after)

    @pl.when(cross_before)
    def _():
        greet(before)

    def up_chunk(p):
        return pl.ds(p * up_per, up_per)

    def load(i, p):
        source, target = ((cur_in, cur), (basis_in, basis), (transfer_in, transfer))[i]
        return pltpu.make_async_copy(
            source.at[up_chunk(p)], target.at[up_chunk(p)], load_sem.at[i, p]
        )

    for p in range(PARTS):
        for i in range(3):
            load(i, p).start()

    def block_load(p):
        span = pl.ds(p * (near_count // PARTS), near_count // PARTS)
        return pltpu.make_async_copy(blocks_in.at[span], blocks.at[span], block_sem.at[p])

    def table_load(p):
        span = pl.ds(p * (table.shape[0] // PARTS), table.shape[0] // PARTS)
        return pltpu.make_async_copy(table_in.at[span], table.at[span], table_sem.at[p])

    for p in range(PARTS):
        block_load(p).start()
    for p in range(PARTS):
        table_load(p).start()

    cap = send_src.shape[2]
    padded = lambda *parts: jnp.concatenate(
        [*parts, jnp.zeros((parts[0].shape[0], 128 - sum(x.shape[1] for x in parts)), jnp.int32)],
        axis=1,
    )
    triple = lambda ref: padded(*(ref[o] for o in range(3)))
    numbers[:n, :] = triple(recv_tgt)
    numbers[n:, :] = triple(recv_type)
    sources[:n, :] = triple(send_src)
    sources[n:, :] = jnp.zeros((8 - n, 128), jnp.int32)
    near_kind = lax.broadcasted_iota(jnp.int32, (1, 128), 1)
    for i, row in enumerate(
        ordered(padded(near_tgt[...]), padded(near_src[...]), near_kind, near_count, leaves, 0)
    ):
        near_rows[i : i + 1, :] = row
    near_copy = pltpu.make_async_copy(near_rows, near_slots, rows_sem.at[0])

    pl.semaphore_wait(
        barrier, n + groups - 2 + jnp.where(cross_after, 1, 0) + jnp.where(cross_before, 1, 0)
    )
    near_copy.start()

    def remote(source, target, sems, at, device):
        return pltpu.make_async_remote_copy(
            src_ref=source,
            dst_ref=target,
            send_sem=sems.at[(0, *at)],
            recv_sem=sems.at[(1, *at)],
            device_id=device,
            device_id_type=MESH,
        )

    def sub_peer(d):
        return (group, lax.rem(me + d, n))

    def rim_copy(side):
        if side == 0:
            return remote(cur_in.at[pl.ds(leaves - halo, halo)], rim.at[0], rim_sem, (0,), after)
        return remote(cur_in.at[pl.ds(0, halo)], rim.at[1], rim_sem, (1,), before)

    def number_copy(d):
        return remote(
            numbers, sub_in.at[me], number_sem, (d - 1,), sub_peer(d)
        )

    def whole_copy(d):
        mine = pl.ds(pl.multiple_of(me * share, share), share)
        return remote(
            shares.at[lax.rem(me + d, n)], whole.at[mine], whole_sem, (d - 1,), sub_peer(d)
        )

    for d in range(1, n):
        number_copy(d).start()
        whole_copy(d).start()

    def source_copy(side):
        there = (up_group, me) if side == 0 else (down_group, me)
        return remote(sources, src_in.at[side], source_sem, (side,), there)

    sends_leaf = [has_up, has_down]
    takes_leaf = [has_down, has_up]
    for side in range(2):
        @pl.when(sends_leaf[side])
        def _(side=side):
            source_copy(side).start()

        @pl.when(jnp.logical_not(takes_leaf[side]))
        def _(side=side):
            src_in[side] = jnp.zeros(src_in.shape[1:], jnp.int32)
            raw[side] = jnp.zeros(raw.shape[1:], F32)

    sends_rim = [has_after, has_before]
    takes_rim = [has_before, has_after]
    late_rim = [me == 0, me == n - 1]
    for side in range(2):
        @pl.when(sends_rim[side] & jnp.logical_not(late_rim[side]))
        def _(side=side):
            rim_copy(side).start()

        @pl.when(jnp.logical_not(takes_rim[side]))
        def _(side=side):
            rim[side] = jnp.zeros(rim.shape[1:], F32)

    def raw_copy(to, p):
        there = {NEXT: (up_group, me), PREV: (down_group, me), SIDE: (group, inner)}[to]
        return remote(coef.at[up_chunk(p)], raw.at[to, up_chunk(p)], raw_sem, (to, p), there)

    sends_raw = [has_up, has_down, is_end]
    takes_raw = [has_down, has_up, is_inner]

    def send_raw(p):
        for to in range(3):
            @pl.when(sends_raw[to])
            def _(to=to):
                raw_copy(to, p).start()

    total = jnp.zeros(mid.shape, F32)
    for p in range(PARTS):
        for i in range(3):
            load(i, p).wait()
        for i in range(up_per):
            l = p * up_per + i
            c = dot3(masked(basis[l], rank[l]), cur[l], TN)
            coef[l] = c
            total += dot3(transfer[l], c, TN)
        if p:
            send_raw(p - 1)
    mid[...] = total
    mine = pl.ds(pl.multiple_of(me * share, share), share)
    whole[mine, :] = shares[me]
    for d in range(1, n):
        whole_copy(d).wait_recv()
    send_raw(PARTS - 1)
    top_part[...] = dot3(whole[...], mid[...])

    def share_copy(d):
        there = lax.rem(me + d, n)
        span = pl.ds(pl.multiple_of(there * share, share), share)
        return remote(top_part.at[span], top_in.at[me], share_sem, (d - 1,), sub_peer(d))

    for d in range(1, n):
        share_copy(d).start()

    def gather(rows, at, store):
        @pl.loop(0, leaves, unroll=2)
        def _(l):
            j = rows[4 * at + 3, l]
            store(l, runs[within(j, runs)] * jnp.where(j >= 0, 1.0, 0.0))

    def in_order(rows, at, number, product):
        unroll = max(u for u in range(1, 7) if number % u == 0)

        def step(i, acc):
            spots = [i * unroll + u for u in range(unroll)]
            results = [product(rows[4 * at, j], rows[4 * at + 1, j]) for j in spots]
            for j, result in zip(spots, results):
                acc = acc * rows[4 * at + 2, j].astype(F32) + result
                runs[j] = acc
            return acc

        lax.fori_loop(0, number // unroll, step, jnp.zeros(runs.shape[1:], F32))

    def near_product(s, k):
        k = within(k, blocks)
        h0, l0 = split(blocks[k, 0])
        h1, l1 = split(blocks[k, 1])
        b = laid_near[within(s, laid_near)]
        return applied(jnp.concatenate([h0, h1], axis=1), jnp.concatenate([l0, l1], axis=1), b)

    def put_near(l, value):
        near_part[l] = value

    for side in range(2):
        @pl.when(takes_leaf[side])
        def _(side=side):
            source_copy(side).wait_recv()

    spot = lax.broadcasted_iota(jnp.int32, (8, 128), 1)
    src_sum[...] = jnp.where(
        spot < cap,
        pltpu.roll(src_in[0], 128 - 2 * cap, 1),
        jnp.where(
            spot < 2 * cap, sources[...] + leaves, pltpu.roll(src_in[1], 2 * cap, 1) + 2 * leaves
        ),
    )

    for p in range(PARTS):
        table_load(p).wait()

    @pl.loop(0, table.shape[0])
    def _(i):
        w = table.shape[3]
        h0, l0 = split(table[i, 0])
        h1, l1 = split(table[i, 1])
        high[i, :, :w] = h0
        high[i, :, w:] = h1
        low[i, :, :w] = l0
        low[i, :, w:] = l1

    ext_src_copy = remote(src_sum, ext_src, ext_src_sem, (), (group, inner))

    @pl.when(is_end)
    def _():
        ext_src_copy.start()
        ext_src[...] = jnp.zeros(ext_src.shape, jnp.int32)

    @pl.loop(0, leaves, unroll=2)
    def _(l):
        lay_out(laid, leaves + l, coef[l])

    sub_in[me] = numbers[...]
    for d in range(1, n):
        number_copy(d).wait_recv()

    def put_rows(at, rows, args):
        for i, row in enumerate(ordered(*args, count, leaves, leaves)):
            rows[4 * at + i : 4 * at + i + 1, :] = row

    for s in range(n):
        args = sub_in[s, pl.ds(me, 1)], src_sum[s : s + 1], sub_in[s, pl.ds(n + me, 1)]
        put_rows(s, far_rows, args)
    far_copy = pltpu.make_async_copy(far_rows, slots, rows_sem.at[1])
    ext_copy_rows = pltpu.make_async_copy(ext_rows, ext_slots, rows_sem.at[2])

    for to in (NEXT, PREV):
        @pl.when(takes_raw[to])
        def _(to=to):
            for p in range(PARTS):
                raw_copy(to, p).wait_recv()

    far_copy.start()

    @pl.loop(0, leaves, unroll=2)
    def _(l):
        lay_out(laid, l, raw[NEXT, l])
        lay_out(laid, 2 * leaves + l, raw[PREV, l])

    far_copy.wait()

    def compute(rows, at, store, role, add=False):
        def product(s, k):
            k = within(k, high)
            return applied(high[k], low[k], store[within(s, store)])

        in_order(rows, at, count, product)

        def put(l, value):
            part[role, l] = part[role, l] + value if add else value

        gather(rows, at, put)

    def chunk(c):
        return pl.ds(c * per, per)

    def end_copy(c):
        return pltpu.make_async_remote_copy(
            src_ref=part.at[FAR, chunk(c)],
            dst_ref=from_end.at[chunk(c)],
            send_sem=out_sem.at[FAR, c],
            recv_sem=end_sem.at[c],
            device_id=(group, inner),
            device_id_type=MESH,
        )

    def other_copy(role, c):
        return pltpu.make_async_remote_copy(
            src_ref=part.at[role, chunk(c)],
            dst_ref=from_other.at[role, chunk(c)],
            send_sem=out_sem.at[role, c],
            recv_sem=other_sem.at[role, c],
            device_id=(group, other),
            device_id_type=MESH,
        )

    def back_copy(c):
        return pltpu.make_async_remote_copy(
            src_ref=part.at[END, chunk(c)],
            dst_ref=from_other.at[1, chunk(c)],
            send_sem=back_sem.at[c],
            recv_sem=other_sem.at[1, c],
            device_id=(group, end),
            device_id_type=MESH,
        )

    def relay(c):
        @pl.when(is_inner)
        def _():
            end_copy(c).wait_recv()
            part[FAR, chunk(c)] += from_end[chunk(c)]
            other_copy(FAR, c).start()

    def relay_back(c):
        @pl.when(is_inner)
        def _():
            other_copy(0, c).wait_recv()
            part[END, chunk(c)] += from_other[0, chunk(c)]
            back_copy(c).start()

    pumped = [0]

    def pump(upto):
        @pl.when(is_end)
        def _():
            for c in range(pumped[0], upto):
                if c >= FLIGHT:
                    end_copy(c - FLIGHT).wait_send()
                end_copy(c).start()

        pumped[0] = upto

    compute(slots, n - 1 - end, laid, FAR)
    pump(FLIGHT)

    def ext_copy(side):
        there = (up_group, me) if side == 0 else (down_group, me)
        return remote(raw.at[SIDE], ext_in.at[side], ext_sem, (side,), there)

    sends_ext = [is_inner & has_up, is_inner & has_down]
    takes_ext = [is_inner & has_down, is_inner & has_up]

    def all_copy(d):
        return remote(
            top_own, tops.at[group], all_sem, (d - 1,), (lax.rem(group + d, groups), me)
        )

    def lay_ext(to, at, ref):
        @pl.loop(0, leaves, unroll=2)
        def _(l):
            lay_out(laid_ext, at * leaves + l, ref[to, l])

    @pl.when(is_inner)
    def _():
        for p in range(PARTS):
            raw_copy(SIDE, p).wait_recv()

    for side in range(2):
        @pl.when(sends_ext[side])
        def _(side=side):
            ext_copy(side).start()

    @pl.when(is_inner)
    def _():
        compute(slots, other, laid, SECOND)
        compute(slots, end, laid, END)

    pump(FLIGHT + 1)
    relay(0)
    compute(slots, me, laid, OWN)
    pump(FLIGHT + 2)
    relay(1)
    top_in[me] = top_part[mine, :]
    for d in range(1, n):
        share_copy(d).wait_recv()
    total = top_in[0]
    for s in range(1, n):
        total += top_in[s]
    top_own[mine, :] = total

    @pl.when(is_inner)
    def _():
        ext_src_copy.wait_recv()
        lay_ext(SIDE, 1, raw)
        for at, to in enumerate((me, other)):
            args = sub_in[to, pl.ds(end, 1)], ext_src[pl.ds(to, 1)], sub_in[to, pl.ds(n + end, 1)]
            put_rows(at, ext_rows, args)

    def top_copy(d):
        return remote(top_own.at[mine], top_own.at[mine], top_sem, (d - 1,), sub_peer(d))

    for d in range(1, n):
        top_copy(d).start()

    ext_copy_rows.start()
    pump(FLIGHT + 3)
    relay(2)
    relay_back(0)
    pump(FLIGHT + 4)
    relay(3)
    relay_back(1)
    pump(FLIGHT + 5)
    for d in range(1, n):
        top_copy(d).wait_recv()
    for d in range(1, groups):
        all_copy(d).start()
    tops[group] = top_own[...]

    relay(4)
    relay_back(2)
    pump(FLIGHT + 6)

    for side in range(2):
        @pl.when(sends_rim[side] & late_rim[side])
        def _(side=side):
            rim_copy(side).start()

    relay(5)
    relay_back(3)
    relay(6)
    relay_back(4)
    relay(7)
    relay_back(5)
    ext_copy_rows.wait()
    for side in range(2):
        @pl.when(takes_ext[side])
        def _(side=side):
            ext_copy(side).wait_recv()
            lay_ext(side, 2 * side, ext_in)

    @pl.when(is_inner)
    def _():
        compute(ext_slots, 1, laid_ext, SECOND, add=True)
        for c in range(AHEAD):
            other_copy(SECOND, c).start()

    relay_back(6)
    for d in range(1, groups):
        all_copy(d).wait_recv()
    field = jnp.zeros((share, mid.shape[1]), F32)
    for k in range(partner.shape[0]):
        p = tops[within(partner[k], tops)]
        field += dot3(coupling[k, 0], p) + dot3(coupling[k, 1], rotated(p))
    field_own[mine, :] = field

    def field_copy(d):
        return remote(field_own.at[mine], field_own.at[mine], field_sem, (d - 1,), sub_peer(d))

    for d in range(1, n):
        field_copy(d).start()

    @pl.when(is_inner)
    def _():
        for c in range(AHEAD, CHUNKS):
            other_copy(SECOND, c).start()

    relay_back(7)

    @pl.when(is_inner)
    def _():
        compute(ext_slots, 0, laid_ext, OWN, add=True)

    for side in range(2):
        @pl.when(takes_rim[side])
        def _(side=side):
            rim_copy(side).wait_recv()

    @pl.loop(0, halo)
    def _(l):
        lay_out(laid_near, l, rim[0, l])
        lay_out(laid_near, halo + leaves + l, rim[1, l])

    @pl.loop(0, leaves, unroll=2)
    def _(l):
        lay_out(laid_near, halo + l, cur[l])

    near_copy.wait()
    for p in range(PARTS):
        block_load(p).wait()
    in_order(near_slots, 0, near_count, near_product)
    gather(near_slots, 0, put_near)

    for d in range(1, n):
        field_copy(d).wait_recv()
    mid[...] = dot3(whole[...], field_own[...], TN)

    @pl.loop(0, leaves, unroll=2)
    def _(l):
        part[OWN, l] += dot3(transfer[l], mid[...])

    def finish(c):
        other_copy(SECOND, c).wait_recv()
        for i in range(per):
            l = c * per + i
            field = part[OWN, l] + from_other[SECOND, l]
            out[l] = dot3(masked(basis[l], rank[l]), field) + near_part[l]

    for c in range(CHUNKS):
        finish(c)

    for side in range(2):
        @pl.when(sends_rim[side])
        def _(side=side):
            rim_copy(side).wait_send()

        @pl.when(sends_leaf[side])
        def _(side=side):
            source_copy(side).wait_send()

        @pl.when(sends_ext[side])
        def _(side=side):
            ext_copy(side).wait_send()

    for to in range(3):
        @pl.when(sends_raw[to])
        def _(to=to):
            for p in range(PARTS):
                raw_copy(to, p).wait_send()

    for d in range(1, n):
        number_copy(d).wait_send()
        whole_copy(d).wait_send()
        share_copy(d).wait_send()
        top_copy(d).wait_send()
        field_copy(d).wait_send()
    for d in range(1, groups):
        all_copy(d).wait_send()

    @pl.when(is_inner)
    def _():
        for c in range(CHUNKS):
            other_copy(FAR, c).wait_send()
            back_copy(c).wait_send()
        for c in range(CHUNKS):
            other_copy(SECOND, c).wait_send()

    @pl.when(is_end)
    def _():
        ext_src_copy.wait_send()
        for c in range(CHUNKS - FLIGHT, CHUNKS):
            end_copy(c).wait_send()


def fields(count, partner, rank, numbers, shares, coupling, cur, basis, transfer, blocks, table):
    leaves, width, cols = cur.shape
    kinds = table.shape[0]
    n = lax.axis_size("sub")
    groups = lax.axis_size("leaf")
    share = width // n
    f32 = lambda *shape: pltpu.VMEM(shape, F32)
    i32 = lambda *shape: pltpu.VMEM(shape, jnp.int32)
    b16 = lambda *shape: pltpu.VMEM(shape, BF16)
    block = lambda *lead: f32(*lead, width, cols)
    dma = lambda *shape: pltpu.SemaphoreType.DMA(shape)
    lists = 4 * n
    lists = -(-lists // 8) * 8
    return pl.pallas_call(
        functools.partial(field_kernel, count),
        in_specs=[SMEM] * 2 + [VMEM] * 7 + [ANY] * 5,
        out_specs=VMEM,
        out_shape=jax.ShapeDtypeStruct((leaves, width, cols), F32),
        scratch_shapes=[
            block(leaves),
            f32(*basis.shape),
            f32(*transfer.shape),
            f32(*blocks.shape),
            f32(*table.shape),
            b16(kinds, width, 2 * width),
            b16(kinds, width, 2 * width),
            block(leaves),
            block(3, leaves),
            block(2, leaves),
            block(2, HALO_L),
            b16(3 * leaves, 2 * width, 2 * cols),
            b16(3 * leaves, 2 * width, 2 * cols),
            b16(leaves + 2 * HALO_L, 2 * width, 2 * cols),
            block(max(count, blocks.shape[0])),
            block(4, leaves),
            block(leaves),
            block(2, leaves),
            block(leaves),
            f32(width, width),
            block(),
            block(),
            f32(n, share, cols),
            block(),
            block(groups),
            block(),
            i32(2 * n, 128),
            i32(8, 128),
            i32(n, 2 * n, 128),
            i32(2, 8, 128),
            i32(8, 128),
            i32(8, 128),
            i32(8, 128),
            i32(lists, 128),
            i32(8, 128),
            pltpu.SMEM((8, 128), jnp.int32),
            pltpu.SMEM((lists, 128), jnp.int32),
            pltpu.SMEM((8, 128), jnp.int32),
            dma(3, PARTS),
            dma(PARTS),
            dma(PARTS),
            dma(3),
            dma(2, 2),
            dma(2, n - 1),
            dma(2, 2),
            dma(2),
            dma(2, 3, PARTS),
            dma(2, 2),
            dma(2, n - 1),
            dma(2, n - 1),
            dma(2, n - 1),
            dma(2, groups - 1),
            dma(2, n - 1),
            dma(2, CHUNKS),
            dma(CHUNKS),
            dma(2, CHUNKS),
            dma(CHUNKS),
        ],
        compiler_params=pltpu.CompilerParams(
            vmem_limit_bytes=67043328, collective_id=0, has_side_effects=True
        ),
        cost_estimate=pl.CostEstimate(
            flops=int(9 * count * 12 * width * width * cols),
            bytes_accessed=20 * 2 ** 20,
            transcendentals=0,
        ),
        name="fields",
    )(partner, rank, *numbers, shares, coupling, cur, basis, transfer, blocks, table)


def per_device(
    currents,
    leaf_basis,
    leaf_rank,
    leaf_transfer,
    top_transfer,
    far_table,
    send_src,
    recv_tgt,
    recv_type,
    top_coupling,
    top_list,
    near_blocks,
    near_tgt,
    near_src,
):
    leaves, panel, _ = leaf_basis.shape
    cols = currents.shape[1]
    out = fields(
        3 * send_src.shape[3],
        top_list[0],
        leaf_rank,
        [send_src[0], recv_tgt[0], recv_type[0], near_tgt, near_src],
        jnp.swapaxes(top_transfer[0], 1, 2),
        top_coupling[0],
        currents.reshape(leaves, panel, cols),
        leaf_basis,
        leaf_transfer,
        near_blocks,
        far_table,
    )
    return out.reshape(leaves * panel, cols)


def solution(mesh):
    placed = (
        P(("leaf", "sub"), None),
        P(("leaf", "sub"), None, None),
        P(("leaf", "sub")),
        P(("leaf", "sub"), None, None),
        P("leaf", None, None, "sub"),
        P(),
        P(("leaf", "sub"), None, None, None),
        P(("leaf", "sub"), None, None, None),
        P(("leaf", "sub"), None, None, None),
        P("leaf", None, None, "sub", None),
        P("leaf", None),
        P(("leaf", "sub"), None, None, None),
        P(("leaf", "sub"), None),
        P(("leaf", "sub"), None),
    )
    return jax.shard_map(
        per_device, mesh=mesh, in_specs=placed, out_specs=P(("leaf", "sub"), None), check_vma=False
    )
```

```python
import functools

import jax
import jax.numpy as jnp
from jax import lax
from jax.experimental import pallas as pl
from jax.experimental.pallas import tpu as pltpu
from jax.sharding import PartitionSpec as P

HALO_L = 4
F32 = jnp.float32
BF16 = jnp.bfloat16
NN = (((1,), (0,)), ((), ()))
TN = (((0,), (0,)), ((), ()))

SMEM = pl.BlockSpec(memory_space=pltpu.SMEM)
VMEM = pl.BlockSpec(memory_space=pltpu.VMEM)
ANY = pl.BlockSpec(memory_space=pl.ANY)
MESH = pl.DeviceIdType.MESH


def split(x):
    high = x.astype(BF16)
    return high, (x - high.astype(F32)).astype(BF16)


def dot(a, b, dims=NN):
    return lax.dot_general(a, b, dims, preferred_element_type=F32)


def dot3(a, b, dims=NN):
    ah, al = split(a)
    bh, bl = split(b)
    return dot(ah, bh, dims) + (dot(ah, bl, dims) + dot(al, bh, dims))


def rotated(c):
    half = c.shape[-1] // 2
    lane = lax.broadcasted_iota(jnp.int32, c.shape, c.ndim - 1)
    turned_c = pltpu.roll(c, half, c.ndim - 1)
    return jnp.where(lane < half, -turned_c, turned_c)


def lay_out(store, at, c):
    rows, cols = c.shape
    high, low = split(c)
    rhigh, rlow = split(rotated(c))
    store[at, :rows, :cols] = high
    store[at, :rows, cols:] = low
    store[at, rows:, :cols] = rhigh
    store[at, rows:, cols:] = rlow


def applied(mh, ml, b):
    cols = b.shape[1] // 2
    p = dot(mh, b)
    return p[:, :cols] + (p[:, cols:] + dot(ml, b[:, :cols]))


def masked(basis, rank):
    lane = lax.broadcasted_iota(jnp.int32, basis.shape, 1)
    return jnp.where(lane < rank, basis, 0.0)


CHUNKS = 8
FLIGHT = 2
AHEAD = 2
PARTS = 4
FAR, SECOND, END, OWN = range(4)
NEXT, PREV, SIDE = range(3)


def ordered(tgt, src, kind, count, leaves, spare):
    rows = -(-count // 8) * 8
    lane = lax.broadcasted_iota(jnp.int32, (rows, 128), 1)
    line = lax.broadcasted_iota(jnp.int32, (rows, 128), 0)
    spot = lax.broadcasted_iota(jnp.int32, (1, 128), 1)
    src = jnp.where(tgt < 0, spare, src).astype(F32)
    key = jnp.where(tgt < 0, leaves, tgt)
    key = jnp.where(spot < count, key, leaves + 1).astype(F32)
    stood = lambda x: jnp.sum(jnp.where(line == lane, x, 0.0), axis=1, keepdims=True)
    key_at = stood(key)
    before = (key < key_at) | ((key == key_at) & (lane < line))
    place = jnp.sum(jnp.where(before, 1.0, 0.0), axis=1, keepdims=True)
    hot = (place == lane.astype(F32)) & (line < count)
    pick = lambda x: jnp.sum(jnp.where(hot, stood(x), 0.0), axis=0, keepdims=True)
    key, src, kind = pick(key), pick(src), pick(kind.astype(F32))
    wide = jnp.broadcast_to(key, (8, 128))
    keep = jnp.where((wide == pltpu.roll(wide, 1, 1))[:1] & (spot > 0), 1.0, 0.0)
    wide = (leaves, 128)
    lane = lax.broadcasted_iota(jnp.int32, wide, 1)
    line = lax.broadcasted_iota(jnp.int32, wide, 0)
    found = (key == line.astype(F32)) & (lane < count)
    last = jnp.max(jnp.where(found, lane.astype(F32), -1.0), axis=1, keepdims=True)
    last = jnp.sum(jnp.where(line == lane, last, 0.0), axis=0, keepdims=True)
    return [x.astype(jnp.int32) for x in (src, kind, keep, last)]


def within(i, ref):
    return jnp.clip(i, 0, ref.shape[0] - 1)


def field_kernel(
    slots_count,
    partner,
    rank,
    send_src,
    recv_tgt,
    recv_type,
    near_tgt,
    near_src,
    shares,
    coupling,
    cur_in,
    basis_in,
    transfer_in,
    blocks_in,
    table_in,
    out,
    cur,
    basis,
    transfer,
    blocks,
    table,
    high,
    low,
    coef,
    raw,
    ext_in,
    rim,
    laid,
    laid_ext,
    laid_near,
    runs,
    part,
    from_end,
    from_other,
    near_part,
    whole,
    mid,
    top_part,
    top_in,
    top_own,
    tops,
    field_own,
    numbers,
    sources,
    sub_in,
    src_in,
    src_sum,
    ext_src,
    near_rows,
    far_rows,
    ext_rows,
    near_slots,
    slots,
    ext_slots,
    load_sem,
    block_sem,
    table_sem,
    rows_sem,
    rim_sem,
    number_sem,
    source_sem,
    ext_src_sem,
    raw_sem,
    ext_sem,
    whole_sem,
    share_sem,
    top_sem,
    all_sem,
    field_sem,
    out_sem,
    end_sem,
    other_sem,
    back_sem,
):
    n = lax.axis_size("sub")
    groups = lax.axis_size("leaf")
    me = lax.axis_index("sub")
    group = lax.axis_index("leaf")
    leaves = cur.shape[0]
    halo = rim.shape[1]
    count = slots_count
    near_count = blocks.shape[0]
    per = leaves // CHUNKS
    up_per = leaves // PARTS
    share = whole.shape[0] // n
    low_side = me < n // 2
    is_end = (me == 0) | (me == n - 1)
    is_inner = (me != 0) & (me != n - 1)
    end = jnp.where(low_side, 0, n - 1)
    inner = jnp.where(low_side, 1, n - 2)
    other = n - 1 - inner
    has_up = group + 1 < groups
    has_down = group > 0
    has_after = has_up | (me < n - 1)
    has_before = has_down | (me > 0)
    up_group = jnp.minimum(group + 1, groups - 1)
    down_group = jnp.maximum(group - 1, 0)
    after = (jnp.where(me < n - 1, group, up_group), lax.rem(me + 1, n))
    before = (jnp.where(me > 0, group, down_group), lax.rem(me + n - 1, n))

    barrier = pltpu.get_barrier_semaphore()

    def greet(device):
        pl.semaphore_signal(barrier, inc=1, device_id=device, device_id_type=MESH)

    for d in range(1, n):
        greet((group, lax.rem(me + d, n)))
    for d in range(1, groups):
        greet((lax.rem(group + d, groups), me))
    cross_after = (me == n - 1) & has_up
    cross_before = (me == 0) & has_down

    @pl.when(cross_after)
    def _():
        greet(after)

    @pl.when(cross_before)
    def _():
        greet(before)

    def up_chunk(p):
        return pl.ds(p * up_per, up_per)

    def load(i, p):
        source, target = ((cur_in, cur), (basis_in, basis), (transfer_in, transfer))[i]
        return pltpu.make_async_copy(
            source.at[up_chunk(p)], target.at[up_chunk(p)], load_sem.at[i, p]
        )

    for p in range(PARTS):
        for i in range(3):
            load(i, p).start()

    def block_load(p):
        span = pl.ds(p * (near_count // PARTS), near_count // PARTS)
        return pltpu.make_async_copy(blocks_in.at[span], blocks.at[span], block_sem.at[p])

    def table_load(p):
        span = pl.ds(p * (table.shape[0] // PARTS), table.shape[0] // PARTS)
        return pltpu.make_async_copy(table_in.at[span], table.at[span], table_sem.at[p])

    for p in range(PARTS):
        block_load(p).start()
    for p in range(PARTS):
        table_load(p).start()

    cap = send_src.shape[2]
    padded = lambda *parts: jnp.concatenate(
        [*parts, jnp.zeros((parts[0].shape[0], 128 - sum(x.shape[1] for x in parts)), jnp.int32)],
        axis=1,
    )
    triple = lambda ref: padded(*(ref[o] for o in range(3)))
    numbers[:n, :] = triple(recv_tgt)
    numbers[n:, :] = triple(recv_type)
    sources[:n, :] = triple(send_src)
    sources[n:, :] = jnp.zeros((8 - n, 128), jnp.int32)
    near_kind = lax.broadcasted_iota(jnp.int32, (1, 128), 1)
    for i, row in enumerate(
        ordered(padded(near_tgt[...]), padded(near_src[...]), near_kind, near_count, leaves, 0)
    ):
        near_rows[i : i + 1, :] = row
    near_copy = pltpu.make_async_copy(near_rows, near_slots, rows_sem.at[0])

    pl.semaphore_wait(
        barrier, n + groups - 2 + jnp.where(cross_after, 1, 0) + jnp.where(cross_before, 1, 0)
    )
    near_copy.start()

    def remote(source, target, sems, at, device):
        return pltpu.make_async_remote_copy(
            src_ref=source,
            dst_ref=target,
            send_sem=sems.at[(0, *at)],
            recv_sem=sems.at[(1, *at)],
            device_id=device,
            device_id_type=MESH,
        )

    def sub_peer(d):
        return (group, lax.rem(me + d, n))

    def rim_copy(side):
        if side == 0:
            return remote(cur_in.at[pl.ds(leaves - halo, halo)], rim.at[0], rim_sem, (0,), after)
        return remote(cur_in.at[pl.ds(0, halo)], rim.at[1], rim_sem, (1,), before)

    def number_copy(d):
        return remote(
            numbers, sub_in.at[me], number_sem, (d - 1,), sub_peer(d)
        )

    def whole_copy(d):
        mine = pl.ds(pl.multiple_of(me * share, share), share)
        return remote(
            shares.at[lax.rem(me + d, n)], whole.at[mine], whole_sem, (d - 1,), sub_peer(d)
        )

    for d in range(1, n):
        number_copy(d).start()
        whole_copy(d).start()

    def source_copy(side):
        there = (up_group, me) if side == 0 else (down_group, me)
        return remote(sources, src_in.at[side], source_sem, (side,), there)

    sends_leaf = [has_up, has_down]
    takes_leaf = [has_down, has_up]
    for side in range(2):
        @pl.when(sends_leaf[side])
        def _(side=side):
            source_copy(side).start()

        @pl.when(jnp.logical_not(takes_leaf[side]))
        def _(side=side):
            src_in[side] = jnp.zeros(src_in.shape[1:], jnp.int32)
            raw[side] = jnp.zeros(raw.shape[1:], F32)

    sends_rim = [has_after, has_before]
    takes_rim = [has_before, has_after]
    late_rim = [me == 0, me == n - 1]
    for side in range(2):
        @pl.when(sends_rim[side] & jnp.logical_not(late_rim[side]))
        def _(side=side):
            rim_copy(side).start()

        @pl.when(jnp.logical_not(takes_rim[side]))
        def _(side=side):
            rim[side] = jnp.zeros(rim.shape[1:], F32)

    def raw_copy(to, p):
        there = {NEXT: (up_group, me), PREV: (down_group, me), SIDE: (group, inner)}[to]
        return remote(coef.at[up_chunk(p)], raw.at[to, up_chunk(p)], raw_sem, (to, p), there)

    sends_raw = [has_up, has_down, is_end]
    takes_raw = [has_down, has_up, is_inner]

    def send_raw(p):
        for to in range(3):
            @pl.when(sends_raw[to])
            def _(to=to):
                raw_copy(to, p).start()

    total = jnp.zeros(mid.shape, F32)
    for p in range(PARTS):
        for i in range(3):
            load(i, p).wait()
        for i in range(up_per):
            l = p * up_per + i
            c = dot3(masked(basis[l], rank[l]), cur[l], TN)
            coef[l] = c
            total += dot3(transfer[l], c, TN)
        if p:
            send_raw(p - 1)
    mid[...] = total
    mine = pl.ds(pl.multiple_of(me * share, share), share)
    whole[mine, :] = shares[me]
    for d in range(1, n):
        whole_copy(d).wait_recv()
    send_raw(PARTS - 1)
    top_part[...] = dot3(whole[...], mid[...])

    def share_copy(d):
        there = lax.rem(me + d, n)
        span = pl.ds(pl.multiple_of(there * share, share), share)
        return remote(top_part.at[span], top_in.at[me], share_sem, (d - 1,), sub_peer(d))

    for d in range(1, n):
        share_copy(d).start()

    def gather(rows, at, store):
        @pl.loop(0, leaves, unroll=2)
        def _(l):
            j = rows[4 * at + 3, l]
            store(l, runs[within(j, runs)] * jnp.where(j >= 0, 1.0, 0.0))

    def in_order(rows, at, number, product):
        unroll = max(u for u in range(1, 7) if number % u == 0)

        def step(i, acc):
            spots = [i * unroll + u for u in range(unroll)]
            results = [product(rows[4 * at, j], rows[4 * at + 1, j]) for j in spots]
            for j, result in zip(spots, results):
                acc = acc * rows[4 * at + 2, j].astype(F32) + result
                runs[j] = acc
            return acc

        lax.fori_loop(0, number // unroll, step, jnp.zeros(runs.shape[1:], F32))

    def near_product(s, k):
        k = within(k, blocks)
        h0, l0 = split(blocks[k, 0])
        h1, l1 = split(blocks[k, 1])
        b = laid_near[within(s, laid_near)]
        return applied(jnp.concatenate([h0, h1], axis=1), jnp.concatenate([l0, l1], axis=1), b)

    def put_near(l, value):
        near_part[l] = value

    for side in range(2):
        @pl.when(takes_leaf[side])
        def _(side=side):
            source_copy(side).wait_recv()

    spot = lax.broadcasted_iota(jnp.int32, (8, 128), 1)
    src_sum[...] = jnp.where(
        spot < cap,
        pltpu.roll(src_in[0], 128 - 2 * cap, 1),
        jnp.where(
            spot < 2 * cap, sources[...] + leaves, pltpu.roll(src_in[1], 2 * cap, 1) + 2 * leaves
        ),
    )

    for p in range(PARTS):
        table_load(p).wait()

    @pl.loop(0, table.shape[0])
    def _(i):
        w = table.shape[3]
        h0, l0 = split(table[i, 0])
        h1, l1 = split(table[i, 1])
        high[i, :, :w] = h0
        high[i, :, w:] = h1
        low[i, :, :w] = l0
        low[i, :, w:] = l1

    ext_src_copy = remote(src_sum, ext_src, ext_src_sem, (), (group, inner))

    @pl.when(is_end)
    def _():
        ext_src_copy.start()
        ext_src[...] = jnp.zeros(ext_src.shape, jnp.int32)

    @pl.loop(0, leaves, unroll=2)
    def _(l):
        lay_out(laid, leaves + l, coef[l])

    sub_in[me] = numbers[...]
    for d in range(1, n):
        number_copy(d).wait_recv()

    def put_rows(at, rows, args):
        for i, row in enumerate(ordered(*args, count, leaves, leaves)):
            rows[4 * at + i : 4 * at + i + 1, :] = row

    for s in range(n):
        args = sub_in[s, pl.ds(me, 1)], src_sum[s : s + 1], sub_in[s, pl.ds(n + me, 1)]
        put_rows(s, far_rows, args)
    far_copy = pltpu.make_async_copy(far_rows, slots, rows_sem.at[1])
    ext_copy_rows = pltpu.make_async_copy(ext_rows, ext_slots, rows_sem.at[2])

    for to in (NEXT, PREV):
        @pl.when(takes_raw[to])
        def _(to=to):
            for p in range(PARTS):
                raw_copy(to, p).wait_recv()

    far_copy.start()

    @pl.loop(0, leaves, unroll=2)
    def _(l):
        lay_out(laid, l, raw[NEXT, l])
        lay_out(laid, 2 * leaves + l, raw[PREV, l])

    far_copy.wait()

    def compute(rows, at, store, role, add=False):
        def product(s, k):
            k = within(k, high)
            return applied(high[k], low[k], store[within(s, store)])

        in_order(rows, at, count, product)

        def put(l, value):
            part[role, l] = part[role, l] + value if add else value

        gather(rows, at, put)

    def chunk(c):
        return pl.ds(c * per, per)

    def end_copy(c):
        return pltpu.make_async_remote_copy(
            src_ref=part.at[FAR, chunk(c)],
            dst_ref=from_end.at[chunk(c)],
            send_sem=out_sem.at[FAR, c],
            recv_sem=end_sem.at[c],
            device_id=(group, inner),
            device_id_type=MESH,
        )

    def other_copy(role, c):
        return pltpu.make_async_remote_copy(
            src_ref=part.at[role, chunk(c)],
            dst_ref=from_other.at[role, chunk(c)],
            send_sem=out_sem.at[role, c],
            recv_sem=other_sem.at[role, c],
            device_id=(group, other),
            device_id_type=MESH,
        )

    def back_copy(c):
        return pltpu.make_async_remote_copy(
            src_ref=part.at[END, chunk(c)],
            dst_ref=from_other.at[1, chunk(c)],
            send_sem=back_sem.at[c],
            recv_sem=other_sem.at[1, c],
            device_id=(group, end),
            device_id_type=MESH,
        )

    def relay(c):
        @pl.when(is_inner)
        def _():
            end_copy(c).wait_recv()
            part[FAR, chunk(c)] += from_end[chunk(c)]
            other_copy(FAR, c).start()

    def relay_back(c):
        @pl.when(is_inner)
        def _():
            other_copy(0, c).wait_recv()
            part[END, chunk(c)] += from_other[0, chunk(c)]
            back_copy(c).start()

    pumped = [0]

    def pump(upto):
        @pl.when(is_end)
        def _():
            for c in range(pumped[0], upto):
                if c >= FLIGHT:
                    end_copy(c - FLIGHT).wait_send()
                end_copy(c).start()

        pumped[0] = upto

    compute(slots, n - 1 - end, laid, FAR)
    pump(FLIGHT)

    def ext_copy(side):
        there = (up_group, me) if side == 0 else (down_group, me)
        return remote(raw.at[SIDE], ext_in.at[side], ext_sem, (side,), there)

    sends_ext = [is_inner & has_up, is_inner & has_down]
    takes_ext = [is_inner & has_down, is_inner & has_up]

    def all_copy(d):
        return remote(
            top_own, tops.at[group], all_sem, (d - 1,), (lax.rem(group + d, groups), me)
        )

    def lay_ext(to, at, ref):
        @pl.loop(0, leaves, unroll=2)
        def _(l):
            lay_out(laid_ext, at * leaves + l, ref[to, l])

    @pl.when(is_inner)
    def _():
        for p in range(PARTS):
            raw_copy(SIDE, p).wait_recv()

    for side in range(2):
        @pl.when(sends_ext[side])
        def _(side=side):
            ext_copy(side).start()

    @pl.when(is_inner)
    def _():
        compute(slots, other, laid, SECOND)
        compute(slots, end, laid, END)

    pump(FLIGHT + 1)
    relay(0)
    compute(slots, me, laid, OWN)
    pump(FLIGHT + 2)
    relay(1)
    top_in[me] = top_part[mine, :]
    for d in range(1, n):
        share_copy(d).wait_recv()
    total = top_in[0]
    for s in range(1, n):
        total += top_in[s]
    top_own[mine, :] = total

    @pl.when(is_inner)
    def _():
        ext_src_copy.wait_recv()
        lay_ext(SIDE, 1, raw)
        for at, to in enumerate((me, other)):
            args = sub_in[to, pl.ds(end, 1)], ext_src[pl.ds(to, 1)], sub_in[to, pl.ds(n + end, 1)]
            put_rows(at, ext_rows, args)

    def top_copy(d):
        return remote(top_own.at[mine], top_own.at[mine], top_sem, (d - 1,), sub_peer(d))

    for d in range(1, n):
        top_copy(d).start()

    ext_copy_rows.start()
    pump(FLIGHT + 3)
    relay(2)
    relay_back(0)
    pump(FLIGHT + 4)
    relay(3)
    relay_back(1)
    pump(FLIGHT + 5)
    for d in range(1, n):
        top_copy(d).wait_recv()
    for d in range(1, groups):
        all_copy(d).start()
    tops[group] = top_own[...]

    relay(4)
    relay_back(2)
    pump(FLIGHT + 6)

    for side in range(2):
        @pl.when(sends_rim[side] & late_rim[side])
        def _(side=side):
            rim_copy(side).start()

    relay(5)
    relay_back(3)
    relay(6)
    relay_back(4)
    relay(7)
    relay_back(5)
    ext_copy_rows.wait()
    for side in range(2):
        @pl.when(takes_ext[side])
        def _(side=side):
            ext_copy(side).wait_recv()
            lay_ext(side, 2 * side, ext_in)

    @pl.when(is_inner)
    def _():
        compute(ext_slots, 1, laid_ext, SECOND, add=True)
        for c in range(AHEAD):
            other_copy(SECOND, c).start()

    relay_back(6)
    for d in range(1, groups):
        all_copy(d).wait_recv()
    field = jnp.zeros((share, mid.shape[1]), F32)
    for k in range(partner.shape[0]):
        p = tops[within(partner[k], tops)]
        field += dot3(coupling[k, 0], p) + dot3(coupling[k, 1], rotated(p))
    field_own[mine, :] = field

    def field_copy(d):
        return remote(field_own.at[mine], field_own.at[mine], field_sem, (d - 1,), sub_peer(d))

    for d in range(1, n):
        field_copy(d).start()

    @pl.when(is_inner)
    def _():
        for c in range(AHEAD, CHUNKS):
            other_copy(SECOND, c).start()

    relay_back(7)

    @pl.when(is_inner)
    def _():
        compute(ext_slots, 0, laid_ext, OWN, add=True)

    for side in range(2):
        @pl.when(takes_rim[side])
        def _(side=side):
            rim_copy(side).wait_recv()

    @pl.loop(0, halo)
    def _(l):
        lay_out(laid_near, l, rim[0, l])
        lay_out(laid_near, halo + leaves + l, rim[1, l])

    @pl.loop(0, leaves, unroll=2)
    def _(l):
        lay_out(laid_near, halo + l, cur[l])

    near_copy.wait()
    for p in range(PARTS):
        block_load(p).wait()
    in_order(near_slots, 0, near_count, near_product)
    gather(near_slots, 0, put_near)

    for d in range(1, n):
        field_copy(d).wait_recv()
    mid[...] = dot3(whole[...], field_own[...], TN)

    @pl.loop(0, leaves, unroll=2)
    def _(l):
        part[OWN, l] += dot3(transfer[l], mid[...])

    def finish(c):
        other_copy(SECOND, c).wait_recv()
        for i in range(per):
            l = c * per + i
            field = part[OWN, l] + from_other[SECOND, l]
            out[l] = dot3(masked(basis[l], rank[l]), field) + near_part[l]

    for c in range(CHUNKS):
        finish(c)

    for side in range(2):
        @pl.when(sends_rim[side])
        def _(side=side):
            rim_copy(side).wait_send()

        @pl.when(sends_leaf[side])
        def _(side=side):
            source_copy(side).wait_send()

        @pl.when(sends_ext[side])
        def _(side=side):
            ext_copy(side).wait_send()

    for to in range(3):
        @pl.when(sends_raw[to])
        def _(to=to):
            for p in range(PARTS):
                raw_copy(to, p).wait_send()

    for d in range(1, n):
        number_copy(d).wait_send()
        whole_copy(d).wait_send()
        share_copy(d).wait_send()
        top_copy(d).wait_send()
        field_copy(d).wait_send()
    for d in range(1, groups):
        all_copy(d).wait_send()

    @pl.when(is_inner)
    def _():
        for c in range(CHUNKS):
            other_copy(FAR, c).wait_send()
            back_copy(c).wait_send()
        for c in range(CHUNKS):
            other_copy(SECOND, c).wait_send()

    @pl.when(is_end)
    def _():
        ext_src_copy.wait_send()
        for c in range(CHUNKS - FLIGHT, CHUNKS):
            end_copy(c).wait_send()


def fields(count, partner, rank, numbers, shares, coupling, cur, basis, transfer, blocks, table):
    leaves, width, cols = cur.shape
    kinds = table.shape[0]
    n = lax.axis_size("sub")
    groups = lax.axis_size("leaf")
    share = width // n
    f32 = lambda *shape: pltpu.VMEM(shape, F32)
    i32 = lambda *shape: pltpu.VMEM(shape, jnp.int32)
    b16 = lambda *shape: pltpu.VMEM(shape, BF16)
    block = lambda *lead: f32(*lead, width, cols)
    dma = lambda *shape: pltpu.SemaphoreType.DMA(shape)
    lists = 4 * n
    lists = -(-lists // 8) * 8
    return pl.pallas_call(
        functools.partial(field_kernel, count),
        in_specs=[SMEM] * 2 + [VMEM] * 7 + [ANY] * 5,
        out_specs=VMEM,
        out_shape=pltpu.VMEM((leaves, width, cols), F32),
        scratch_shapes=[
            block(leaves),
            f32(*basis.shape),
            f32(*transfer.shape),
            f32(*blocks.shape),
            f32(*table.shape),
            b16(kinds, width, 2 * width),
            b16(kinds, width, 2 * width),
            block(leaves),
            block(3, leaves),
            block(2, leaves),
            block(2, HALO_L),
            b16(3 * leaves, 2 * width, 2 * cols),
            b16(3 * leaves, 2 * width, 2 * cols),
            b16(leaves + 2 * HALO_L, 2 * width, 2 * cols),
            block(max(count, blocks.shape[0])),
            block(4, leaves),
            block(leaves),
            block(2, leaves),
            block(leaves),
            f32(width, width),
            block(),
            block(),
            f32(n, share, cols),
            block(),
            block(groups),
            block(),
            i32(2 * n, 128),
            i32(8, 128),
            i32(n, 2 * n, 128),
            i32(2, 8, 128),
            i32(8, 128),
            i32(8, 128),
            i32(8, 128),
            i32(lists, 128),
            i32(8, 128),
            pltpu.SMEM((8, 128), jnp.int32),
            pltpu.SMEM((lists, 128), jnp.int32),
            pltpu.SMEM((8, 128), jnp.int32),
            dma(3, PARTS),
            dma(PARTS),
            dma(PARTS),
            dma(3),
            dma(2, 2),
            dma(2, n - 1),
            dma(2, 2),
            dma(2),
            dma(2, 3, PARTS),
            dma(2, 2),
            dma(2, n - 1),
            dma(2, n - 1),
            dma(2, n - 1),
            dma(2, groups - 1),
            dma(2, n - 1),
            dma(2, CHUNKS),
            dma(CHUNKS),
            dma(2, CHUNKS),
            dma(CHUNKS),
        ],
        compiler_params=pltpu.CompilerParams(
            vmem_limit_bytes=60 * 1024 * 1024, collective_id=0, has_side_effects=True
        ),
        cost_estimate=pl.CostEstimate(
            flops=int(9 * count * 12 * width * width * cols),
            bytes_accessed=20 * 2 ** 20,
            transcendentals=0,
        ),
        name="fields",
    )(partner, rank, *numbers, shares, coupling, cur, basis, transfer, blocks, table)


def per_device(
    currents,
    leaf_basis,
    leaf_rank,
    leaf_transfer,
    top_transfer,
    far_table,
    send_src,
    recv_tgt,
    recv_type,
    top_coupling,
    top_list,
    near_blocks,
    near_tgt,
    near_src,
):
    leaves, panel, _ = leaf_basis.shape
    cols = currents.shape[1]
    out = fields(
        3 * send_src.shape[3],
        top_list[0],
        leaf_rank,
        [send_src[0], recv_tgt[0], recv_type[0], near_tgt, near_src],
        jnp.swapaxes(top_transfer[0], 1, 2),
        top_coupling[0],
        currents.reshape(leaves, panel, cols),
        leaf_basis,
        leaf_transfer,
        near_blocks,
        far_table,
    )
    return out.reshape(leaves * panel, cols)


def solution(mesh):
    placed = (
        P(("leaf", "sub"), None),
        P(("leaf", "sub"), None, None),
        P(("leaf", "sub")),
        P(("leaf", "sub"), None, None),
        P("leaf", None, None, "sub"),
        P(),
        P(("leaf", "sub"), None, None, None),
        P(("leaf", "sub"), None, None, None),
        P(("leaf", "sub"), None, None, None),
        P("leaf", None, None, "sub", None),
        P("leaf", None),
        P(("leaf", "sub"), None, None, None),
        P(("leaf", "sub"), None),
        P(("leaf", "sub"), None),
    )
    return jax.shard_map(
        per_device, mesh=mesh, in_specs=placed, out_specs=P(("leaf", "sub"), None), check_vma=False
    )
```
